128 devices in a mesh: lat: 4 (over y), lon: 4 (over z), mesh: 8 (over x, core).
Axes of the slice: x: 4, y: 4, z: 4, core: 2. Of those that a mesh axis runs over, the one named last changes fastest.
Arguments:
- grid_latent: bfloat16 [131072, 512], P(('lat', 'lon', 'mesh')), may hold values from -24 to 24
- target: bfloat16 [131072, 84], P(('lat', 'lon', 'mesh')), may hold values from -6 to 6
- area: float32 [131072], P(('lat', 'lon', 'mesh')), may hold values from 0.05 to 1
- mesh_latent: bfloat16 [40960, 512], P(('lat', 'lon', 'mesh')), may hold values from -6 to 6
- node_gain: float32 [512], replicated, may hold values from 0.1 to 1.9
- w_enc: bfloat16 [512, 512], replicated, may hold values from -0.25 to 0.25
- w_up: bfloat16 [512, 512], replicated, may hold values from -0.25 to 0.25
- w_down: bfloat16 [512, 512], replicated, may hold values from -0.25 to 0.25
- w_msg: bfloat16 [512, 512], replicated, may hold values from -0.25 to 0.25
- w_dec: bfloat16 [512, 512], replicated, may hold values from -0.25 to 0.25
- w_out: bfloat16 [512, 84], replicated, may hold values from -0.25 to 0.25
- enc_cell: int32 [128, 3, 3, 8, 21], P(('lat', 'lon', 'mesh')), may hold values from 0 to 1023
- enc_live: int32 [128, 3, 3, 8], P(('lat', 'lon', 'mesh')), may hold values from 1 to 21, as said below
- enc_weight: float32 [128, 3, 3, 8, 21], P(('lat', 'lon', 'mesh')), may hold values from 0.2 to 1
- enc_node: int32 [128, 3, 3, 8, 21], P(('lat', 'lon', 'mesh')), may hold values from 0 to 319
- dec_node: int32 [128, 3, 3, 8, 32], P(('lat', 'lon', 'mesh')), may hold values from 0 to 319
- dec_cell: int32 [128, 3, 3, 8, 32], P(('lat', 'lon', 'mesh')), may hold values from 0 to 1023
- dec_weight: float32 [128, 3, 3, 8, 32], P(('lat', 'lon', 'mesh')), may hold values from 0.2 to 1
Outputs:
- grid_grad: float32 [131072, 512], P(('lat', 'lon', 'mesh'))
- grad_enc: float32 [512, 512], P(('lat', 'lon', 'mesh'))
- grad_up: float32 [512, 512], P(('lat', 'lon', 'mesh'))
- grad_down: float32 [512, 512], P(('lat', 'lon', 'mesh'))
- grad_msg: float32 [512, 512], P(('lat', 'lon', 'mesh'))
- grad_dec: float32 [512, 512], P(('lat', 'lon', 'mesh'))
- grad_out: float32 [512, 84], P(('lat', 'lon', 'mesh'))
The draws below stay inside these ranges and needn't reach their ends.
Inputs may be any that keep to these rules, and one draw needn't show every extreme that they name: Slots 0 to enc_live - 1 of a bucket are edges, the others padding; in every draw some mesh owner receives 21 live slots in every bucket addressed to it. `enc_cell`: local cell indices. `enc_node`: local node indices. `dec_node`: local node indices. `dec_cell`: local cell indices.
All inputs are finite; a program needn't handle non-finite values.
Results may differ from the reference program's by a relative error of at most 0.0085.
Values may be sent and summed in bfloat16 or wider, within the bound.
A program may use at most 128 MiB of HBM per device.

```python
import math
import jax
import jax.numpy as jnp
from jax import lax

W = 512
OUT = 84
CELL_DEV = 1024
NODE_DEV = 320
SLOT_E = 21
SLOT_D = 32
CELLS = 131072
NODES = 40960
N_LAT = 4
N_LON = 4
N_MESH = 8
DEVICES = 128


def draw_enc_live(key, part):
    key_busy, key_chosen, key_lesser = jax.random.split(jax.random.fold_in(key, 7), 3)
    busy_owner = jax.random.randint(key_busy, (DEVICES,), 0, 4) == 0
    chosen = jax.random.randint(key_chosen, (), 0, DEVICES)
    busy_owner = busy_owner | (jnp.arange(DEVICES) == chosen)
    device_ids = jnp.arange(DEVICES, dtype=jnp.int32)
    lat_of = device_ids // (N_LON * N_MESH)
    lon_of = device_ids // N_MESH % N_LON
    offsets = jnp.arange(3, dtype=jnp.int32) - 1
    owner_parts = jnp.arange(N_MESH, dtype=jnp.int32)
    lat_at = (lat_of[:, None] + offsets[None, :]) % N_LAT
    lon_at = (lon_of[:, None] + offsets[None, :]) % N_LON
    destination = (lat_at[:, :, None, None] * N_LON + lon_at[:, None, :, None]) * N_MESH + owner_parts[None, None, None, :]
    lesser = jax.random.randint(key_lesser, (DEVICES, 3, 3, N_MESH), 1, SLOT_E // 2 + 1)
    return jnp.where(busy_owner[destination], SLOT_E, lesser).astype(jnp.int32)


def touch_ends(entries, rng, smallest, largest):
    longest = entries.shape.index(max(entries.shape))
    spots = []
    for shift in (0, 1):
        where = [jax.random.randint(jax.random.fold_in(rng, axis), (), 0, length) for axis, length in enumerate(entries.shape)]
        where[longest] = (where[longest] + shift) % entries.shape[longest]
        spots.append(tuple(where))
    return entries.at[spots[0]].set(smallest).at[spots[1]].set(largest)


def with_spikes(array, rng, source, target, parts, factor):
    owner, partner = [(jnp.arange(array.shape[axis_at]) // (array.shape[axis_at] // parts)).reshape([-1 if axis == axis_at else 1 for axis in range(array.ndim)]) for axis_at in (source, target)]
    chosen = jax.random.permutation(rng, parts)[partner]
    strong = (owner == chosen) | (owner == (partner + parts // 2) % parts)
    return jnp.where(strong, factor * array, array)


def block_scale(own_key, extent, cuts, least, high):
    def one(position, shards_of):
        draws = jax.random.uniform(jax.random.fold_in(jax.random.fold_in(own_key, 6), position), (shards_of,), jnp.float32, least / len(cuts), high / len(cuts))
        return jnp.repeat(jnp.exp(draws), extent[position] // shards_of).reshape((-1,) + (1,) * (len(extent) - position - 1))

    factor_of = one(*cuts[0])
    for cut in cuts[1:]:
        factor_of = factor_of * one(*cut)
    return factor_of


def gaussian(key, dims, deviation, reach, shards=(), held_as=jnp.bfloat16):
    drawn = deviation * jax.random.normal(key, dims, jnp.float32)
    if shards:
        drawn = drawn * block_scale(key, dims, shards, -0.22, 0.18)
    return jnp.clip(drawn, -reach, reach).astype(held_as)


def bell_draw_with(own_key, extent, scale, limit, cuts, heavy, held_as=jnp.bfloat16):
    result = scale * jax.random.normal(own_key, extent, jnp.float32)
    if cuts:
        result = result * block_scale(own_key, extent, cuts, -0.22, 0.18)
    return jnp.clip(with_spikes(result, jax.random.fold_in(own_key, 3), *heavy), -limit, limit).astype(held_as)


def setup_inputs(seed: int = 0) -> dict:
    splits = jax.random.split(jax.random.key(seed), 19)
    grid_latent = bell_draw_with(splits[0], (CELLS, W), 1.0, 24.0, ((0, 128),), (0, 1, 128, 5.5))
    target = gaussian(splits[1], (CELLS, OUT), 1.0, 6.0, ((0, 128),))
    area = jnp.clip(jnp.exp(math.log(1.0) - 2.9957323 * jax.random.uniform(splits[2], (CELLS,), jnp.float32) ** block_scale(splits[2], (CELLS,), ((0, 128),), -0.2, 0.2)), 0.05, 1.0)
    mesh_latent = gaussian(splits[3], (NODES, W), 1.0, 6.0, ((0, 128),))
    node_gain = jnp.clip(1.0 + 0.18 * jax.random.normal(splits[4], (W,), jnp.float32), 0.1, 1.9)
    w_enc = gaussian(splits[5], (W, W), W ** -0.5, 0.25)
    w_up = gaussian(splits[6], (W, W), W ** -0.5, 0.25)
    w_down = gaussian(splits[7], (W, W), W ** -0.5, 0.25)
    w_msg = gaussian(splits[8], (W, W), W ** -0.5, 0.25)
    w_dec = gaussian(splits[9], (W, W), W ** -0.5, 0.25)
    w_out = gaussian(splits[10], (W, OUT), W ** -0.5, 0.25)
    enc_cell = touch_ends(jax.random.randint(splits[11], (DEVICES, 3, 3, N_MESH, SLOT_E), 0, CELL_DEV), jax.random.fold_in(splits[11], 1), 0, CELL_DEV - 1).astype(jnp.int32)
    enc_live = draw_enc_live(jax.random.fold_in(splits[18], 71), 0)
    enc_weight = jnp.clip(jnp.exp(math.log(1.0) - 1.609438 * jax.random.uniform(splits[13], (DEVICES, 3, 3, N_MESH, SLOT_E), jnp.float32) ** block_scale(splits[13], (DEVICES, 3, 3, N_MESH, SLOT_E), ((0, 128),), -0.2, 0.2)), 0.2, 1.0)
    enc_node = touch_ends(jax.random.randint(splits[14], (DEVICES, 3, 3, N_MESH, SLOT_E), 0, NODE_DEV), jax.random.fold_in(splits[14], 1), 0, NODE_DEV - 1).astype(jnp.int32)
    dec_node = touch_ends(jax.random.randint(splits[15], (DEVICES, 3, 3, N_MESH, SLOT_D), 0, NODE_DEV), jax.random.fold_in(splits[15], 1), 0, NODE_DEV - 1).astype(jnp.int32)
    dec_cell = touch_ends(jax.random.randint(splits[16], (DEVICES, 3, 3, N_MESH, SLOT_D), 0, CELL_DEV), jax.random.fold_in(splits[16], 1), 0, CELL_DEV - 1).astype(jnp.int32)
    dec_weight = jnp.clip(jnp.exp(math.log(1.0) - 1.609438 * jax.random.uniform(splits[17], (DEVICES, 3, 3, N_MESH, SLOT_D), jnp.float32) ** block_scale(splits[17], (DEVICES, 3, 3, N_MESH, SLOT_D), ((0, 128),), -0.2, 0.2)), 0.2, 1.0)
    return dict(grid_latent=grid_latent, target=target, area=area, mesh_latent=mesh_latent, node_gain=node_gain, w_enc=w_enc, w_up=w_up, w_down=w_down, w_msg=w_msg, w_dec=w_dec, w_out=w_out, enc_cell=enc_cell, enc_live=enc_live, enc_weight=enc_weight, enc_node=enc_node, dec_node=dec_node, dec_cell=dec_cell, dec_weight=dec_weight)


def matmul(left, right):
    return jnp.dot(left, right, preferred_element_type=jnp.float32)

def contract(left, right):
    return lax.dot_general(left, right, (((0,), (0,)), ((), ())), preferred_element_type=jnp.float32)

def silu_slope(argument):
    sigmoid_value = jax.nn.sigmoid(argument)
    return sigmoid_value * (1.0 + argument * (1.0 - sigmoid_value))

def node_forward(node_state, node_gain, w_up, w_down):
    inv_rms = lax.rsqrt(lax.optimization_barrier(jnp.mean(node_state * node_state, axis=-1, keepdims=True)) + 1e-05)
    normed = (node_state * inv_rms * node_gain).astype(jnp.bfloat16)
    activation = matmul(normed, w_up)
    hidden = jax.nn.silu(activation).astype(jnp.bfloat16)
    updated = node_state + matmul(hidden, w_down)
    return (updated, inv_rms, normed, activation, hidden)

def node_backward(back_node, node_state, node_gain, w_up, w_down, inv_rms, normed, activation, hidden):
    back_node_half = back_node.astype(jnp.bfloat16)
    grad_down = contract(hidden, back_node_half)
    back_hidden = matmul(back_node_half, w_down.T)
    back_act = (back_hidden * silu_slope(activation)).astype(jnp.bfloat16)
    grad_up = contract(normed, back_act)
    back_norm = matmul(back_act, w_up.T) * node_gain
    mean_term = lax.optimization_barrier(jnp.mean(node_state * back_norm, axis=-1, keepdims=True))
    back_state = back_node + inv_rms * back_norm - node_state * inv_rms ** 3 * mean_term
    return (back_state, grad_up, grad_down)

def linked(lat_of, lon_of, offsets, step_sign):
    owner_parts = jnp.arange(N_MESH, dtype=jnp.int32)
    lat_at = (lat_of[:, None] + step_sign * offsets[None, :]) % N_LAT
    lon_at = (lon_of[:, None] + step_sign * offsets[None, :]) % N_LON
    return ((lat_at[:, :, None, None] * N_LON + lon_at[:, None, :, None]) * N_MESH + owner_parts[None, None, None, :]).astype(jnp.int32)

def reference(grid_latent, target, area, mesh_latent, node_gain, w_enc, w_up, w_down, w_msg, w_dec, w_out, enc_cell, enc_live, enc_weight, enc_node, dec_node, dec_cell, dec_weight):
    features = grid_latent.shape[1]
    device_ids = jnp.arange(DEVICES, dtype=jnp.int32)
    lat_of = device_ids // (N_LON * N_MESH)
    lon_of = device_ids // N_MESH % N_LON
    mesh_of = device_ids % N_MESH
    offsets = jnp.arange(3, dtype=jnp.int32) - 1
    source = linked(lat_of, lon_of, offsets, -1)
    destination = linked(lat_of, lon_of, offsets, 1)
    reach_up = lat_of[:, None] + offsets[None, :]
    send_ok = (reach_up >= 0) & (reach_up < N_LAT)
    reach_down = lat_of[:, None] - offsets[None, :]
    recv_ok = (reach_down >= 0) & (reach_down < N_LAT)
    slot_index = jnp.arange(SLOT_E, dtype=jnp.int32)
    edge_scale = jnp.where((slot_index < enc_live[..., None]) & send_ok[:, :, None, None, None], enc_weight, jnp.float32(0.0))
    dec_scale = jnp.where(recv_ok[:, :, None, None, None], dec_weight, jnp.float32(0.0))
    row_grid = jnp.arange(3, dtype=jnp.int32)[:, None, None]
    col_grid = jnp.arange(3, dtype=jnp.int32)[None, :, None]
    projected = matmul(grid_latent, w_enc).astype(jnp.bfloat16)

    def encode(device_id):
        anchor = source[device_id]
        cell_ids = enc_cell[anchor, row_grid, col_grid, mesh_of[device_id]]
        slot_scale = edge_scale[anchor, row_grid, col_grid, mesh_of[device_id]]
        row_block = projected[anchor[..., None] * CELL_DEV + cell_ids]
        scaled = (slot_scale[..., None] * row_block.astype(jnp.float32)).astype(jnp.bfloat16)
        scaled = lax.optimization_barrier(scaled)
        return jax.ops.segment_sum(scaled.reshape(-1, features).astype(jnp.float32), enc_node[device_id].reshape(-1), num_segments=NODE_DEV)
    aggregate = lax.map(encode, device_ids).reshape(-1, features)
    node_state = mesh_latent.astype(jnp.float32) + aggregate
    updated, inv_rms, normed, activation, hidden = node_forward(node_state, node_gain, w_up, w_down)
    node_half = updated.astype(jnp.bfloat16)

    def pull_ids(device_id):
        anchor = source[device_id]
        node_ids = dec_node[anchor, row_grid, col_grid, mesh_of[device_id]]
        return (anchor[..., None] * NODE_DEV + node_ids).reshape(-1)

    def decode(device_id):
        message = jax.nn.silu(matmul(node_half[pull_ids(device_id)], w_msg))
        weighted = dec_scale[device_id].reshape(-1)[:, None] * message
        return jax.ops.segment_sum(weighted, dec_cell[device_id].reshape(-1), num_segments=CELL_DEV)
    gathered = lax.map(decode, device_ids).reshape(-1, features).astype(jnp.bfloat16)
    blended = grid_latent.astype(jnp.float32) + matmul(gathered, w_dec)
    blended_half = blended.astype(jnp.bfloat16)
    output = matmul(blended_half, w_out)
    residual = (area[:, None] * (output - target.astype(jnp.float32))).astype(jnp.bfloat16)
    grad_out = contract(blended_half, residual) / CELL_DEV
    back_blend = matmul(residual, w_out.T)
    back_half = back_blend.astype(jnp.bfloat16)
    grad_dec = contract(gathered, back_half) / CELL_DEV
    back_gather = matmul(back_half, w_dec.T).astype(jnp.bfloat16)

    def decode_back(running, device_id):
        grad_sum, back_node = running
        node_ids = pull_ids(device_id)
        row_block = node_half[node_ids]
        preact = matmul(row_block, w_msg)
        cell_ids = device_id * CELL_DEV + dec_cell[device_id].reshape(-1)
        back_message = dec_scale[device_id].reshape(-1)[:, None] * back_gather[cell_ids].astype(jnp.float32)
        back_preact = (back_message * silu_slope(preact)).astype(jnp.bfloat16)
        grad_sum = grad_sum + contract(row_block, back_preact)
        back_pulled = matmul(back_preact, w_msg.T).astype(jnp.bfloat16)
        back_pulled = lax.optimization_barrier(back_pulled)
        back_node = back_node.at[node_ids].add(back_pulled.astype(jnp.float32))
        return ((grad_sum, back_node), None)
    start = (jnp.zeros((features, features), jnp.float32), jnp.zeros((DEVICES * NODE_DEV, features), jnp.float32))
    (grad_msg, back_node), unused = lax.scan(decode_back, start, device_ids)
    grad_msg = grad_msg / CELL_DEV
    back_state, grad_up, grad_down = node_backward(back_node, node_state, node_gain, w_up, w_down, inv_rms, normed, activation, hidden)
    back_state_half = back_state.astype(jnp.bfloat16)

    def encode_back(device_id):
        ahead = destination[device_id]
        node_ids = enc_node[ahead, row_grid, col_grid, mesh_of[device_id]]
        row_block = back_state_half[ahead[..., None] * NODE_DEV + node_ids]
        weighted = edge_scale[device_id][..., None] * row_block.astype(jnp.float32)
        return jax.ops.segment_sum(weighted.reshape(-1, features), enc_cell[device_id].reshape(-1), num_segments=CELL_DEV)
    back_proj = lax.map(encode_back, device_ids).reshape(-1, features).astype(jnp.bfloat16)
    grad_enc = contract(grid_latent, back_proj) / CELL_DEV
    grid_grad = back_blend + matmul(back_proj, w_enc.T)
    return (grid_grad, grad_enc, grad_up / CELL_DEV, grad_down / CELL_DEV, grad_msg, grad_dec, grad_out)
```

```python
import jax
import jax.numpy as jnp
from jax import lax
from jax.experimental import pallas as pl
from jax.experimental.pallas import tpu as pltpu
from jax.sharding import PartitionSpec as P

AXES = ("lat", "lon", "mesh")
MESH_ID = pl.DeviceIdType.MESH
W = 512
CELLS = 1024
NODES = 320
SE = 21
SEP = 24
SD = 32
EROWS = 8 * SEP
DROWS = 8 * SD
T_ENC_CELL, T_ENC_NODE, T_DEC_NODE, T_DEC_CELL, T_ENC_SCALE, T_DEC_SCALE, T_AREA = (
    0,
    9,
    18,
    27,
    36,
    45,
    54,
)
VMEM_LIMIT = 67043328
BF = jnp.bfloat16
F32 = jnp.float32


def dot(a, b):
    return jnp.dot(a, b, preferred_element_type=F32)


def dot_nt(a, b):
    return lax.dot_general(a, b, (((1,), (1,)), ((), ())), preferred_element_type=F32)


def dot_tn(a, b):
    return lax.dot_general(a, b, (((0,), (0,)), ((), ())), preferred_element_type=F32)


def sigmoid(x):
    return 0.5 * jnp.tanh(0.5 * x) + 0.5


def slope(x):
    s = sigmoid(x)
    return s * (1.0 + x * (1.0 - s))


def kernel(
    enc_cell_in,
    enc_node_in,
    dec_node_in,
    dec_cell_in,
    enc_weight_in,
    dec_weight_in,
    enc_live_in,
    area_in,
    target_t_in,
    w_out_t_in,
    node_gain_in,
    grid_latent_in,
    mesh_latent_in,
    w_enc_in,
    w_up_in,
    w_down_in,
    w_msg_in,
    w_dec_in,
    grid_grad,
    g_enc,
    g_up,
    g_down,
    g_msg,
    g_dec,
    g_out,
    enc_cell,
    enc_node,
    dec_node,
    dec_cell,
    enc_weight,
    dec_weight,
    enc_live,
    area,
    target_t,
    w_out_t,
    node_gain,
    grid_latent,
    mesh_latent,
    w_enc,
    w_up,
    w_down,
    w_msg,
    w_dec,
    target,
    pad,
    table,
    cols,
    es,
    ed,
    ds_,
    dd,
    bs,
    bd,
    fs,
    fd,
    acc_n,
    acc_c,
    gath,
    blend,
    bhalf,
    bgath,
    resid,
    wo,
    nstate,
    act,
    normed,
    hidden,
    nhalf,
    prew,
    aggb,
    ga,
    la_c,
    ha,
    la_y,
    ha2,
    la_z,
    gb,
    lb_c,
    hu,
    lu_y,
    hu2,
    lu_z,
    hv,
    lv_z,
    hv2,
    lv_y,
    hm,
    lm,
    ssem,
    rsem,
    gs,
    gr,
    ls,
):
    la, lo, me = lax.axis_index("lat"), lax.axis_index("lon"), lax.axis_index("mesh")
    core = lax.rem(me, 2)

    def device(dla, dlo, part):
        return {"lat": lax.rem(la + dla, 4), "lon": lax.rem(lo + dlo, 4), "mesh": part}

    barrier = pltpu.get_barrier_semaphore()
    peers = 0
    for p in range(3):
        for q in range(3):
            for d in range(8):
                if p == 1 and q == 1 and d == 0:
                    continue
                pl.semaphore_signal(
                    barrier,
                    inc=1,
                    device_id=device(p + 3, q + 3, lax.rem(me + d, 8)),
                    device_id_type=MESH_ID,
                )
                peers += 1
    for dla, dlo in ((2, 0), (0, 2)):
        pl.semaphore_signal(
            barrier, inc=1, device_id=device(dla, dlo, me), device_id_type=MESH_ID
        )
        peers += 1

    loads = []
    for i, (src, dst) in enumerate(
        (
            (enc_cell_in, enc_cell),
            (enc_node_in, enc_node),
            (dec_node_in, dec_node),
            (dec_cell_in, dec_cell),
            (enc_weight_in, enc_weight),
            (dec_weight_in, dec_weight),
            (enc_live_in, enc_live),
            (area_in, area),
            (target_t_in, target_t),
            (w_out_t_in, w_out_t),
            (node_gain_in, node_gain),
            (grid_latent_in, grid_latent),
            (mesh_latent_in, mesh_latent),
            (w_enc_in, w_enc),
            (w_up_in, w_up),
            (w_down_in, w_down),
            (w_msg_in, w_msg),
            (w_dec_in, w_dec),
        )
    ):
        loads.append(pltpu.make_async_copy(src, dst, ls.at[i]))
        loads[i].start()

    for copy in loads[:11]:
        copy.wait()

    table[...] = jnp.zeros_like(table)
    pad[...] = jnp.zeros_like(pad)

    def fill(k, carry):
        def put(block, value, slots, stride):
            pad[:, 0:slots] = value
            row = pad[0:1, :]
            for m in range(1, 8):
                row = row + pltpu.roll(pad[m : m + 1, :], m * stride, axis=1)
            table[pl.ds(block + k, 1), :] = row

        put(T_DEC_NODE, dec_node[k].astype(F32), SD, SD)
        put(T_DEC_CELL, dec_cell[k].astype(F32), SD, SD)
        put(T_DEC_SCALE, dec_weight[k], SD, SD)
        pad[...] = jnp.zeros_like(pad)
        put(T_ENC_CELL, enc_cell[k].astype(F32), SE, SEP)
        put(T_ENC_NODE, enc_node[k].astype(F32), SE, SEP)
        here = lax.broadcasted_iota(jnp.int32, (8, 8), 0) == lax.broadcasted_iota(
            jnp.int32, (8, 8), 1
        )
        live = jnp.sum(jnp.where(here, enc_live[k].astype(F32), 0.0), axis=1, keepdims=True)
        slot = lax.broadcasted_iota(jnp.int32, (8, SE), 1).astype(F32)
        put(T_ENC_SCALE, jnp.where(slot < live, enc_weight[k], 0.0), SE, SEP)
        return carry

    lax.fori_loop(0, 9, fill, 0)
    for b in range(4):
        table[T_AREA + b : T_AREA + b + 1, 0:128] = area[2 * b : 2 * b + 1, :]
        table[T_AREA + b : T_AREA + b + 1, 128:256] = area[2 * b + 1 : 2 * b + 2, :]
    cols[...] = table[...].T
    wo[...] = jnp.zeros_like(wo)
    wo[0:84, :] = w_out_t[...]
    target[...] = jnp.zeros_like(target)
    target[0:84, :] = target_t[...].astype(F32)
    loads[11].wait()

    def column(block, k, rows):
        turned = pltpu.roll(cols[...], lax.rem(128 - (block + k), 128), axis=1)
        return turned[0:rows, 0:1]

    def pick(block, k, rows, width):
        index = column(block, k, rows).astype(jnp.int32)
        return (index == lax.broadcasted_iota(jnp.int32, (rows, width), 1)).astype(F32).astype(BF)

    def place(block, k, rows, width):
        index = table[pl.ds(block + k, 1), :][:, 0:width].astype(jnp.int32)
        return (index == lax.broadcasted_iota(jnp.int32, (rows, width), 0)).astype(F32)

    def chunk_of(t):
        return lax.rem(4 * t + 8, 9)

    def valid(k, sign):
        at = la + sign * (k // 3 - 1)
        return (at >= 0) & (at < 4)

    def send(phase, k, src, dst, sign):
        dla = k // 3 - 1
        dlo = lax.rem(k, 3) - 1
        for d in (4, 3, 5, 2, 6, 1, 7, 0):
            part = lax.rem(me + d, 8)
            copy = pltpu.make_async_remote_copy(
                src_ref=src.at[k * 8 + part],
                dst_ref=dst.at[k * 8 + me],
                send_sem=ssem.at[phase, k],
                recv_sem=rsem.at[phase, k],
                device_id=device(sign * dla + 4, sign * dlo + 4, part),
                device_id_type=MESH_ID,
            )
            if d == 0:
                pl.when(k != 4)(copy.start)
            else:
                copy.start()

    def await_bytes(sem, phase, k, buf):
        whole = buf.at[pl.ds(k * 8, 8)]
        most = buf.at[pl.ds(k * 8, 7)]

        @pl.when(k != 4)
        def _():
            pltpu.make_async_copy(whole, whole, sem.at[phase, k]).wait()

        @pl.when(k == 4)
        def _():
            pltpu.make_async_copy(most, most, sem.at[phase, k]).wait()

    def own(k, src, dst):
        @pl.when(k == 4)
        def _():
            dst[4 * 8 + me] = src[4 * 8 + me]

    def put_rows(buf, k, rows_f32, slots):
        for m in range(8):
            buf[k * 8 + m] = rows_f32[m * slots : (m + 1) * slots, :].astype(BF)

    def get_rows(buf, k, slots):
        return buf[pl.ds(k * 8, 8)].astype(F32).reshape(8 * slots, W)

    def loop(body, first=0, last=9):
        def step(t, carry):
            body(chunk_of(t))
            return carry

        lax.fori_loop(first, last, step, 0)

    def enc_make(k):
        @pl.when(valid(k, 1))
        def _():
            rows = dot(pick(T_ENC_CELL, k, EROWS, CELLS), grid_latent[...])
            put_rows(es, k, rows * column(T_ENC_SCALE, k, EROWS), SEP)

    loop(enc_make, 0, 3)
    pl.semaphore_wait(barrier, peers)

    def enc_send(k):
        @pl.when(valid(k, 1))
        def _():
            send(0, k, es, ed, 1)
            own(k, es, ed)

    def enc_both(k):
        enc_make(k)
        enc_send(k)

    loop(enc_send, 0, 3)
    loop(enc_both, 3, 9)

    acc_n[...] = jnp.zeros_like(acc_n)

    def enc_take(k):
        @pl.when(valid(k, -1))
        def _():
            await_bytes(rsem, 0, k, ed)
            rows = get_rows(ed, k, SEP).astype(BF)
            acc_n[...] += dot(place(T_ENC_NODE, k, NODES, EROWS).astype(BF), rows)

    loop(enc_take)

    for copy in loads[12:]:
        copy.wait()
    aggb[...] = acc_n[...].astype(BF)
    state = mesh_latent[...].astype(F32) + dot(aggb[...], w_enc[...])
    nstate[...] = state
    inv_rms = lax.rsqrt(jnp.mean(state * state, axis=-1, keepdims=True) + 1e-05)
    normed[...] = (state * inv_rms * node_gain[...]).astype(BF)
    activation = dot(normed[...], w_up[...])
    act[...] = activation
    hidden[...] = (activation * sigmoid(activation)).astype(BF)
    nhalf[...] = (nstate[...] + dot(hidden[...], w_down[...])).astype(BF)
    prew[...] = dot(nhalf[...], w_msg[...]).astype(BF)

    def dec_send(k):
        @pl.when(valid(k, 1))
        def _():
            put_rows(ds_, k, dot(pick(T_DEC_NODE, k, DROWS, NODES), prew[...]), SD)
            send(1, k, ds_, dd, 1)
            own(k, ds_, dd)

    loop(dec_send)
    acc_c[...] = jnp.zeros_like(acc_c)

    def dec_take(k):
        @pl.when(valid(k, -1))
        def _():
            await_bytes(rsem, 1, k, dd)
            pre = get_rows(dd, k, SD)
            rows = (column(T_DEC_SCALE, k, DROWS) * (pre * sigmoid(pre))).astype(BF)
            acc_c[...] += dot(place(T_DEC_CELL, k, CELLS, DROWS).astype(BF), rows)

    loop(dec_take)

    for b in range(4):
        at = pl.ds(b * 256, 256)
        gathered = acc_c[at, :].astype(BF)
        gath[at, :] = gathered
        blended = (grid_latent[at, :].astype(F32) + dot(gathered, w_dec[...])).astype(BF)
        blend[at, :] = blended
        output = dot_nt(blended, wo[...])
        weight = cols[0:256, T_AREA + b : T_AREA + b + 1]
        residual = (weight * (output - target[:, at].T)).astype(BF)
        resid[at, :] = residual
        back = dot(residual, wo[...])
        grid_grad[at, :] = back
        half = back.astype(BF)
        bhalf[at, :] = half
        bgath[at, :] = dot_nt(half, w_dec[...]).astype(BF)

    def back_send(k):
        @pl.when(valid(k, -1))
        def _():
            pre = get_rows(dd, k, SD)
            rows = dot(pick(T_DEC_CELL, k, DROWS, CELLS), bgath[...])
            put_rows(bs, k, rows * column(T_DEC_SCALE, k, DROWS) * slope(pre), SD)
            send(2, k, bs, bd, -1)
            own(k, bs, bd)

    loop(back_send)

    def to(src, dst, slot, where):
        copy = pltpu.make_async_remote_copy(
            src_ref=src,
            dst_ref=dst,
            send_sem=gs.at[slot],
            recv_sem=gr.at[slot],
            device_id=where,
            device_id_type=MESH_ID,
        )
        copy.start()
        sent.append(copy)
        return copy

    def over_lat(src, dst, slot):
        return [
            to(src.at[lax.rem(la + d, 4)], dst.at[d - 1], slot + d, device(d, 0, me))
            for d in (2, 1, 3)
        ]

    def over_lon(src, dst, slot):
        return [
            to(src.at[lax.rem(lo + d, 4)], dst.at[d - 1], slot + d, device(0, d, me))
            for d in (2, 1, 3)
        ]

    def arrived(copies):
        for copy in copies:
            copy.wait_recv()

    sent = []
    partner = device(0, 0, me + 1 - 2 * core)
    scale = 1.0 / CELLS
    grad = (dot_tn(gath[...], bhalf[...]) * scale).astype(BF)
    ga[0] = grad[:, 0:384]
    ga[1, :, 0:128] = grad[:, 384:512]
    ga[1, :, 128:256] = (dot_tn(blend[...], resid[...]) * scale).astype(BF)
    ga[1, :, 256:384] = jnp.zeros((W, 128), BF)
    arrived([to(ga.at[1 - core], la_c, 0, partner)])
    for j in range(4):
        rows = pl.ds(j * 128, 128)
        ha[j] = (ga[core, rows, :].astype(F32) + la_c[rows, :].astype(F32)).astype(BF)
    wait_a = over_lat(ha, la_y, 0)

    acc_n[...] = jnp.zeros_like(acc_n)

    def back_take(k):
        @pl.when(valid(k, 1))
        def _():
            await_bytes(rsem, 2, k, bd)
            rows = get_rows(bd, k, SD).astype(BF)
            acc_n[...] += dot(place(T_DEC_NODE, k, NODES, DROWS).astype(BF), rows)

    loop(back_take)

    back_pre = acc_n[...].astype(BF)
    back_node = dot_nt(back_pre, w_msg[...])
    back_node_half = back_node.astype(BF)
    back_act = (dot_nt(back_node_half, w_down[...]) * slope(act[...])).astype(BF)
    back_norm = dot_nt(back_act, w_up[...]) * node_gain[...]
    state = nstate[...]
    inv_rms = lax.rsqrt(jnp.mean(state * state, axis=-1, keepdims=True) + 1e-05)
    mean_term = jnp.mean(state * back_norm, axis=-1, keepdims=True)
    back_state = back_node + inv_rms * back_norm - state * (inv_rms * inv_rms * inv_rms * mean_term)
    back_half = back_state.astype(BF)
    prew[...] = dot_nt(back_half, w_enc[...]).astype(BF)

    def enc_back_send(k):
        @pl.when(valid(k, -1))
        def _():
            put_rows(fs, k, dot(pick(T_ENC_NODE, k, EROWS, NODES), prew[...]), SEP)
            send(3, k, fs, fd, -1)
            own(k, fs, fd)

    gb[0, :, 0:512] = (dot_tn(nhalf[...], back_pre) * scale).astype(BF)
    gb[0, :, 512:1024] = (dot_tn(hidden[...], back_node_half) * scale).astype(BF)
    gb[1, :, 0:512] = (dot_tn(normed[...], back_act) * scale).astype(BF)
    gb[1, :, 512:1024] = (dot_tn(aggb[...], back_half) * scale).astype(BF)
    wait_b = [to(gb.at[1 - core], lb_c, 4, partner)]

    loop(enc_back_send, 0, 3)

    arrived(wait_b)
    for j in range(4):
        rows = pl.ds(j * 128, 128)
        both = gb[core, rows, :].astype(F32) + lb_c[rows, :].astype(F32)
        hu[j] = both[:, 0:512].astype(BF)
        for i in range(4):
            hv[i, j] = both[i * 32 : (i + 1) * 32, 512:1024].astype(BF)
    wait_u = over_lat(hu, lu_y, 4)
    wait_v = over_lon(hv, lv_z, 8)
    arrived(wait_a)
    total = ha[la].astype(F32) + la_y[0].astype(F32) + la_y[1].astype(F32) + la_y[2].astype(F32)
    for j in range(4):
        ha2[j] = total[j * 32 : (j + 1) * 32, :].astype(BF)
    wait_a = over_lon(ha2, la_z, 12)

    loop(enc_back_send, 3, 6)

    arrived(wait_u)
    total = hu[la].astype(F32) + lu_y[0].astype(F32) + lu_y[1].astype(F32) + lu_y[2].astype(F32)
    for j in range(4):
        hu2[j] = total[j * 32 : (j + 1) * 32, :].astype(BF)
    wait_u = over_lon(hu2, lu_z, 16)
    arrived(wait_v)
    for j in range(4):
        total = hv[lo, j].astype(F32) + lv_z[0, j].astype(F32)
        hv2[j] = (total + lv_z[1, j].astype(F32) + lv_z[2, j].astype(F32)).astype(BF)
    wait_v = over_lat(hv2, lv_y, 20)

    loop(enc_back_send, 6, 9)

    def finished(own_part, landed):
        total = own_part.astype(F32) + landed[0].astype(F32)
        return total + landed[1].astype(F32) + landed[2].astype(F32)

    arrived(wait_u)
    arrived(wait_v)
    arrived(wait_a)
    for at, total in (
        (0, finished(hu2[lo], lu_z)),
        (512, finished(hv2[la], lv_y)),
        (1024, finished(ha2[lo], la_z)),
    ):
        for j in range(8):
            hm[j, :, at : at + total.shape[1]] = total[j * 4 : (j + 1) * 4, :]
    wait_m = []
    for d in (4, 3, 5, 2, 6, 1, 7):
        part = lax.rem(me + d, 8)
        wait_m.append(to(hm.at[part], lm.at[d - 1], 24 + d, device(0, 0, part)))

    def enc_back_take(k):
        @pl.when(valid(k, 1))
        def _():
            await_bytes(rsem, 3, k, fd)
            rows = get_rows(fd, k, SEP).astype(BF)
            weight = table[pl.ds(T_ENC_SCALE + k, 1), :][:, 0:EROWS]
            spread = (place(T_ENC_CELL, k, CELLS, EROWS) * weight).astype(BF)
            grid_grad[...] += dot(spread, rows)

    loop(enc_back_take)

    arrived(wait_m)
    same = hm[me]
    other = lm[0]
    same = same + lm[1] + lm[3] + lm[5]
    other = other + lm[2] + lm[4] + lm[6]
    low = jnp.where(core == 0, same, other)
    high = jnp.where(core == 0, other, same)
    g_msg[...] = low[:, 0:512]
    g_down[...] = low[:, 512:1024]
    g_dec[:, 0:384] = low[:, 1024:1408]
    g_up[...] = high[:, 0:512]
    g_enc[...] = high[:, 512:1024]
    g_dec[:, 384:512] = high[:, 1024:1152]
    g_out[...] = high[:, 1152 : 1152 + 84]

    for c in sent:
        c.wait_send()

    def drain(k):
        @pl.when(valid(k, 1))
        def _():
            await_bytes(ssem, 0, k, es)
            await_bytes(ssem, 1, k, ds_)

        @pl.when(valid(k, -1))
        def _():
            await_bytes(ssem, 2, k, bs)
            await_bytes(ssem, 3, k, fs)

    loop(drain)


def scratch():
    v = pltpu.VMEM
    return [
        v((9, 8, SE), jnp.int32),
        v((9, 8, SE), jnp.int32),
        v((9, 8, SD), jnp.int32),
        v((9, 8, SD), jnp.int32),
        v((9, 8, SE), F32),
        v((9, 8, SD), F32),
        v((9, 1, 8), jnp.int32),
        v((8, 128), F32),
        v((84, CELLS), BF),
        v((84, W), BF),
        v((1, W), F32),
        v((CELLS, W), BF),
        v((NODES, W), BF),
        v((W, W), BF),
        v((W, W), BF),
        v((W, W), BF),
        v((W, W), BF),
        v((W, W), BF),
        v((128, CELLS), F32),
        v((8, 256), F32),
        v((128, 256), F32),
        v((256, 128), F32),
        v((72, SEP, W), BF),
        v((72, SEP, W), BF),
        v((72, SD, W), BF),
        v((72, SD, W), BF),
        v((72, SD, W), BF),
        v((72, SD, W), BF),
        v((72, SEP, W), BF),
        v((72, SEP, W), BF),
        v((NODES, W), F32),
        v((CELLS, W), F32),
        v((CELLS, W), BF),
        v((CELLS, W), BF),
        v((CELLS, W), BF),
        v((CELLS, W), BF),
        v((CELLS, 128), BF),
        v((128, W), BF),
        v((NODES, W), F32),
        v((NODES, W), F32),
        v((NODES, W), BF),
        v((NODES, W), BF),
        v((NODES, W), BF),
        v((NODES, W), BF),
        v((NODES, W), BF),
        v((2, W, 384), BF),
        v((W, 384), BF),
        v((4, 128, 384), BF),
        v((3, 128, 384), BF),
        v((4, 32, 384), BF),
        v((3, 32, 384), BF),
        v((2, W, 1024), BF),
        v((W, 1024), BF),
        v((4, 128, 512), BF),
        v((3, 128, 512), BF),
        v((4, 32, 512), BF),
        v((3, 32, 512), BF),
        v((4, 4, 32, 512), BF),
        v((3, 4, 32, 512), BF),
        v((4, 32, 512), BF),
        v((3, 32, 512), BF),
        v((8, 4, 1408), F32),
        v((7, 4, 1408), F32),
        pltpu.SemaphoreType.DMA((4, 9)),
        pltpu.SemaphoreType.DMA((4, 9)),
        pltpu.SemaphoreType.DMA((32,)),
        pltpu.SemaphoreType.DMA((32,)),
        pltpu.SemaphoreType.DMA((18,)),
    ]


def on_device(
    grid_latent,
    target,
    area,
    mesh_latent,
    node_gain,
    w_enc,
    w_up,
    w_down,
    w_msg,
    w_dec,
    w_out,
    enc_cell,
    enc_live,
    enc_weight,
    enc_node,
    dec_node,
    dec_cell,
    dec_weight,
):
    vm = pl.BlockSpec(memory_space=pltpu.VMEM)
    small = jax.ShapeDtypeStruct((4, W), F32)
    any_space = pl.BlockSpec(memory_space=pl.ANY)
    shapes = (jax.ShapeDtypeStruct((CELLS, W), F32),) + (small,) * 5
    shapes += (jax.ShapeDtypeStruct((4, 84), F32),)
    outs = pl.pallas_call(
        kernel,
        out_shape=shapes,
        in_specs=[any_space] * 18,
        out_specs=(vm,) * 7,
        scratch_shapes=scratch(),
        compiler_params=pltpu.CompilerParams(
            collective_id=0, has_side_effects=True, vmem_limit_bytes=VMEM_LIMIT
        ),
        name="step",
    )(
        enc_cell.reshape(9, 8, SE),
        enc_node.reshape(9, 8, SE),
        dec_node.reshape(9, 8, SD),
        dec_cell.reshape(9, 8, SD),
        enc_weight.reshape(9, 8, SE),
        dec_weight.reshape(9, 8, SD),
        enc_live.reshape(9, 1, 8),
        area.reshape(8, 128),
        target.T,
        w_out.T,
        node_gain.reshape(1, W),
        grid_latent,
        mesh_latent,
        w_enc,
        w_up,
        w_down,
        w_msg,
        w_dec,
    )
    return pl.pallas_call(
        finish,
        out_shape=shapes,
        in_specs=[any_space] * 7,
        out_specs=(any_space,) * 7,
        scratch_shapes=[
            pltpu.VMEM((CELLS, W), F32),
            pltpu.VMEM((5, 4, W), F32),
            pltpu.VMEM((4, 84), F32),
            pltpu.SemaphoreType.DMA((10,)),
            pltpu.SemaphoreType.DMA((10,)),
        ],
        compiler_params=pltpu.CompilerParams(vmem_limit_bytes=VMEM_LIMIT),
        name="finish",
    )(*outs)


def finish(*refs):
    grid, small, head, arrive, leave = refs[14:]
    parts = [
        (refs[0].at[rows], grid.at[rows], refs[7].at[rows])
        for rows in (pl.ds(b * 256, 256) for b in range(4))
    ]
    parts += [(refs[i], small.at[i - 1], refs[7 + i]) for i in range(1, 6)]
    parts.append((refs[6], head, refs[13]))
    inward = [pltpu.make_async_copy(a, b, arrive.at[i]) for i, (a, b, c) in enumerate(parts)]
    outward = [pltpu.make_async_copy(b, c, leave.at[i]) for i, (a, b, c) in enumerate(parts)]
    for copy in inward:
        copy.start()
    for first, second in zip(inward, outward):
        first.wait()
        second.start()
    for copy in outward:
        copy.wait()


def solution(mesh):
    rows = P(AXES, None)
    slots = P(AXES, None, None, None, None)
    in_specs = (
        rows,
        rows,
        P(AXES),
        rows,
        P(),
        P(),
        P(),
        P(),
        P(),
        P(),
        P(),
        slots,
        P(AXES, None, None, None),
        slots,
        slots,
        slots,
        slots,
        slots,
    )
    return jax.shard_map(
        on_device, mesh=mesh, in_specs=in_specs, out_specs=(rows,) * 7, check_vma=False
    )
```

```python
import jax
import jax.numpy as jnp
from jax import lax
from jax.experimental import pallas as pl
from jax.experimental.pallas import tpu as pltpu
from jax.sharding import PartitionSpec as P

AXES = ("lat", "lon", "mesh")
MESH_ID = pl.DeviceIdType.MESH
W = 512
CELLS = 1024
NODES = 320
SE = 21
SEP = 24
SD = 32
EROWS = 8 * SEP
DROWS = 8 * SD
T_ENC_CELL, T_ENC_NODE, T_DEC_NODE, T_DEC_CELL, T_ENC_SCALE, T_DEC_SCALE, T_AREA = (
    0,
    9,
    18,
    27,
    36,
    45,
    54,
)
VMEM_LIMIT = 67043328
BF = jnp.bfloat16
F32 = jnp.float32


def dot(a, b):
    return jnp.dot(a, b, preferred_element_type=F32)


def dot_nt(a, b):
    return lax.dot_general(a, b, (((1,), (1,)), ((), ())), preferred_element_type=F32)


def dot_tn(a, b):
    return lax.dot_general(a, b, (((0,), (0,)), ((), ())), preferred_element_type=F32)


def sigmoid(x):
    return 0.5 * jnp.tanh(0.5 * x) + 0.5


def slope(x):
    s = sigmoid(x)
    return s * (1.0 + x * (1.0 - s))


def kernel(
    enc_cell_in,
    enc_node_in,
    dec_node_in,
    dec_cell_in,
    enc_weight_in,
    dec_weight_in,
    enc_live_in,
    area_in,
    target_t_in,
    w_out_t_in,
    node_gain_in,
    grid_latent_in,
    mesh_latent_in,
    w_enc_in,
    w_up_in,
    w_down_in,
    w_msg_in,
    w_dec_in,
    grid_grad,
    g_enc,
    g_up,
    g_down,
    g_msg,
    g_dec,
    g_out,
    enc_cell,
    enc_node,
    dec_node,
    dec_cell,
    enc_weight,
    dec_weight,
    enc_live,
    area,
    target_t,
    w_out_t,
    node_gain,
    grid_latent,
    mesh_latent,
    w_enc,
    w_up,
    w_down,
    w_msg,
    w_dec,
    target,
    pad,
    table,
    cols,
    by_part,
    far_part,
    far_rows,
    far_out,
    backw,
    es,
    ed,
    ds_,
    dd,
    bs,
    bd,
    fs,
    fd,
    acc_n,
    acc_c,
    gath,
    blend,
    bhalf,
    bgath,
    resid,
    wo,
    nstate,
    act,
    normed,
    hidden,
    nhalf,
    prew,
    aggb,
    ga,
    la_c,
    ha,
    la_y,
    ha2,
    la_z,
    gb,
    lb_c,
    hu,
    lu_y,
    hu2,
    lu_z,
    hv,
    lv_z,
    hv2,
    lv_y,
    hm,
    lm,
    ssem,
    rsem,
    gs,
    gr,
    ls,
):
    la, lo, me = lax.axis_index("lat"), lax.axis_index("lon"), lax.axis_index("mesh")
    core = lax.rem(me, 2)
    far_same = lax.rem(me + 4, 8)
    far_other = far_same + 1 - 2 * core

    def device(dla, dlo, part):
        return {"lat": lax.rem(la + dla, 4), "lon": lax.rem(lo + dlo, 4), "mesh": part}

    barrier = pltpu.get_barrier_semaphore()
    peers = 0
    for p in range(3):
        for q in range(3):
            for d in range(8):
                if p == 1 and q == 1 and d == 0:
                    continue
                pl.semaphore_signal(
                    barrier,
                    inc=1,
                    device_id=device(p + 3, q + 3, lax.rem(me + d, 8)),
                    device_id_type=MESH_ID,
                )
                peers += 1
    for dla, dlo in ((2, 0), (0, 2)):
        pl.semaphore_signal(
            barrier, inc=1, device_id=device(dla, dlo, me), device_id_type=MESH_ID
        )
        peers += 1

    loads = []
    for i, (src, dst) in enumerate(
        (
            (enc_cell_in, enc_cell),
            (enc_node_in, enc_node),
            (dec_node_in, dec_node),
            (dec_cell_in, dec_cell),
            (enc_weight_in, enc_weight),
            (dec_weight_in, dec_weight),
            (enc_live_in, enc_live),
            (area_in, area),
            (target_t_in, target_t),
            (w_out_t_in, w_out_t),
            (node_gain_in, node_gain),
            (grid_latent_in, grid_latent),
            (mesh_latent_in, mesh_latent),
            (w_enc_in, w_enc),
            (w_up_in, w_up),
            (w_down_in, w_down),
            (w_msg_in, w_msg),
            (w_dec_in, w_dec),
        )
    ):
        loads.append(pltpu.make_async_copy(src, dst, ls.at[i]))
        loads[i].start()

    for copy in loads[:11]:
        copy.wait()

    table[...] = jnp.zeros_like(table)
    pad[...] = jnp.zeros_like(pad)

    def fill(k, carry):
        def put(block, value, slots, stride):
            pad[:, 0:slots] = value
            row = pad[0:1, :]
            for m in range(1, 8):
                row = row + pltpu.roll(pad[m : m + 1, :], m * stride, axis=1)
            table[pl.ds(block + k, 1), :] = row

        put(T_DEC_NODE, dec_node[k].astype(F32), SD, SD)
        for m in range(8):
            by_part[m, pl.ds(k, 1), :] = pad[m : m + 1, 0:128]
        put(T_DEC_CELL, dec_cell[k].astype(F32), SD, SD)
        put(T_DEC_SCALE, dec_weight[k], SD, SD)
        pad[...] = jnp.zeros_like(pad)
        put(T_ENC_CELL, enc_cell[k].astype(F32), SE, SEP)
        put(T_ENC_NODE, enc_node[k].astype(F32), SE, SEP)
        here = lax.broadcasted_iota(jnp.int32, (8, 8), 0) == lax.broadcasted_iota(
            jnp.int32, (8, 8), 1
        )
        live = jnp.sum(jnp.where(here, enc_live[k].astype(F32), 0.0), axis=1, keepdims=True)
        slot = lax.broadcasted_iota(jnp.int32, (8, SE), 1).astype(F32)
        put(T_ENC_SCALE, jnp.where(slot < live, enc_weight[k], 0.0), SE, SEP)
        return carry

    lax.fori_loop(0, 9, fill, 0)
    for b in range(4):
        table[T_AREA + b : T_AREA + b + 1, 0:128] = area[2 * b : 2 * b + 1, :]
        table[T_AREA + b : T_AREA + b + 1, 128:256] = area[2 * b + 1 : 2 * b + 2, :]
    cols[...] = table[...].T
    wo[...] = jnp.zeros_like(wo)
    wo[0:84, :] = w_out_t[...]
    target[...] = jnp.zeros_like(target)
    target[0:84, :] = target_t[...].astype(F32)
    loads[11].wait()

    def column(block, k, rows):
        turned = pltpu.roll(cols[...], lax.rem(128 - (block + k), 128), axis=1)
        return turned[0:rows, 0:1]

    def pick(block, k, rows, width):
        index = column(block, k, rows).astype(jnp.int32)
        return (index == lax.broadcasted_iota(jnp.int32, (rows, width), 1)).astype(F32).astype(BF)

    def place(block, k, rows, width):
        index = table[pl.ds(block + k, 1), :][:, 0:width].astype(jnp.int32)
        return (index == lax.broadcasted_iota(jnp.int32, (rows, width), 0)).astype(F32)

    def chunk_of(t):
        return lax.rem(4 * t + 8, 9)

    def valid(k, sign):
        at = la + sign * (k // 3 - 1)
        return (at >= 0) & (at < 4)

    def to(src, dst, slot, where):
        copy = pltpu.make_async_remote_copy(
            src_ref=src,
            dst_ref=dst,
            send_sem=gs.at[slot],
            recv_sem=gr.at[slot],
            device_id=where,
            device_id_type=MESH_ID,
        )
        copy.start()
        sent.append(copy)
        return copy

    def arrived(copies):
        for copy in copies:
            copy.wait_recv()

    sent = []
    partner = device(0, 0, me + 1 - 2 * core)

    def send(phase, k, src, dst, sign):
        dla = k // 3 - 1
        dlo = lax.rem(k, 3) - 1
        for d in (4, 3, 5, 2, 6, 1, 7, 0):
            if phase == 1 and d in (3, 4, 5):
                continue
            part = lax.rem(me + d, 8)
            copy = pltpu.make_async_remote_copy(
                src_ref=src.at[k * 8 + part],
                dst_ref=dst.at[k * 8 + me],
                send_sem=ssem.at[phase, k],
                recv_sem=rsem.at[phase, k],
                device_id=device(sign * dla + 4, sign * dlo + 4, part),
                device_id_type=MESH_ID,
            )
            if d == 0:
                pl.when(k != 4)(copy.start)
            else:
                copy.start()
        if phase == 1:
            part = lax.rem(me + 3 + 2 * core, 8)
            pltpu.make_async_remote_copy(
                src_ref=src.at[k * 8 + part],
                dst_ref=dst.at[k * 8 + me],
                send_sem=ssem.at[phase, k],
                recv_sem=rsem.at[phase, k],
                device_id=device(sign * dla + 4, sign * dlo + 4, part),
                device_id_type=MESH_ID,
            ).start()

    def await_bytes(sem, phase, k, buf):
        whole = buf.at[pl.ds(k * 8, 8)]
        most = buf.at[pl.ds(k * 8, 5 if phase == 1 else 7)]

        @pl.when(k != 4)
        def _():
            pltpu.make_async_copy(whole, whole, sem.at[phase, k]).wait()

        @pl.when(k == 4)
        def _():
            pltpu.make_async_copy(most, most, sem.at[phase, k]).wait()

    def own(k, src, dst):
        @pl.when(k == 4)
        def _():
            dst[4 * 8 + me] = src[4 * 8 + me]

    def put_rows(buf, k, rows_f32, slots):
        for m in range(8):
            buf[k * 8 + m] = rows_f32[m * slots : (m + 1) * slots, :].astype(BF)

    def get_rows(buf, k, slots):
        return buf[pl.ds(k * 8, 8)].astype(F32).reshape(8 * slots, W)

    def loop(body, first=0, last=9):
        def step(t, carry):
            body(chunk_of(t))
            return carry

        lax.fori_loop(first, last, step, 0)

    def enc_make(k):
        @pl.when(valid(k, 1))
        def _():
            rows = dot(pick(T_ENC_CELL, k, EROWS, CELLS), grid_latent[...])
            put_rows(es, k, rows * column(T_ENC_SCALE, k, EROWS), SEP)

    loop(enc_make, 0, 3)
    pl.semaphore_wait(barrier, peers)

    def enc_send(k):
        @pl.when(valid(k, 1))
        def _():
            send(0, k, es, ed, 1)
            own(k, es, ed)

    def enc_both(k):
        enc_make(k)
        enc_send(k)

    loop(enc_send, 0, 3)
    far_tables = [
        to(by_part.at[far_same], far_part.at[0], 27, device(0, 0, far_same)),
        to(by_part.at[far_other], far_part.at[1], 28, device(0, 0, far_other)),
    ]
    loop(enc_both, 3, 9)

    acc_n[...] = jnp.zeros_like(acc_n)

    def enc_take(k):
        @pl.when(valid(k, -1))
        def _():
            await_bytes(rsem, 0, k, ed)
            rows = get_rows(ed, k, SEP).astype(BF)
            acc_n[...] += dot(place(T_ENC_NODE, k, NODES, EROWS).astype(BF), rows)

    loop(enc_take)

    for copy in loads[12:]:
        copy.wait()
    aggb[...] = acc_n[...].astype(BF)
    state = mesh_latent[...].astype(F32) + dot(aggb[...], w_enc[...])
    nstate[...] = state
    inv_rms = lax.rsqrt(jnp.mean(state * state, axis=-1, keepdims=True) + 1e-05)
    normed[...] = (state * inv_rms * node_gain[...]).astype(BF)
    activation = dot(normed[...], w_up[...])
    act[...] = activation
    hidden[...] = (activation * sigmoid(activation)).astype(BF)
    nhalf[...] = (nstate[...] + dot(hidden[...], w_down[...])).astype(BF)
    prew[...] = dot(nhalf[...], w_msg[...]).astype(BF)

    def dec_send(k):
        @pl.when(valid(k, 1))
        def _():
            put_rows(ds_, k, dot(pick(T_DEC_NODE, k, DROWS, NODES), prew[...]), SD)
            send(1, k, ds_, dd, 1)
            own(k, ds_, dd)

    far_block = to(prew, far_rows.at[0], 29, device(0, 0, far_same))
    loop(dec_send)

    def relay(i, source):
        turned = far_part[i].T
        index = jnp.concatenate([turned[0:SD, k : k + 1] for k in range(9)], axis=0)
        width = lax.broadcasted_iota(jnp.int32, (9 * SD, NODES), 1)
        chosen = (index.astype(jnp.int32) == width).astype(F32).astype(BF)
        rows = dot(chosen, far_rows[i]).astype(BF)
        for k in range(9):
            far_out[i * 9 + k] = rows[k * SD : (k + 1) * SD, :]

        def relay_send(k):
            @pl.when(valid(k, 1) & (k != 4))
            def _():
                pltpu.make_async_remote_copy(
                    src_ref=far_out.at[i * 9 + k],
                    dst_ref=dd.at[k * 8 + source],
                    send_sem=ssem.at[1, k],
                    recv_sem=rsem.at[1, k],
                    device_id=device(k // 3 + 3, lax.rem(k, 3) + 3, me),
                    device_id_type=MESH_ID,
                ).start()

        loop(relay_send)
        dd[4 * 8 + source] = far_out[i * 9 + 4]

    arrived(far_tables)
    arrived([far_block])
    far_block = to(far_rows.at[0], far_rows.at[1], 30, partner)
    relay(0, far_same)
    arrived([far_block])
    relay(1, far_other)
    acc_c[...] = jnp.zeros_like(acc_c)

    def dec_take(k):
        @pl.when(valid(k, -1))
        def _():
            await_bytes(rsem, 1, k, dd)
            pre = get_rows(dd, k, SD)
            rows = (column(T_DEC_SCALE, k, DROWS) * (pre * sigmoid(pre))).astype(BF)
            acc_c[...] += dot(place(T_DEC_CELL, k, CELLS, DROWS).astype(BF), rows)

    loop(dec_take)

    for b in range(4):
        at = pl.ds(b * 256, 256)
        gathered = acc_c[at, :].astype(BF)
        gath[at, :] = gathered
        blended = (grid_latent[at, :].astype(F32) + dot(gathered, w_dec[...])).astype(BF)
        blend[at, :] = blended
        output = dot_nt(blended, wo[...])
        weight = cols[0:256, T_AREA + b : T_AREA + b + 1]
        residual = (weight * (output - target[:, at].T)).astype(BF)
        resid[at, :] = residual
        back = dot(residual, wo[...])
        grid_grad[at, :] = back
        half = back.astype(BF)
        bhalf[at, :] = half
        bgath[at, :] = dot_nt(half, w_dec[...]).astype(BF)

    def back_send(k):
        @pl.when(valid(k, -1))
        def _():
            pre = get_rows(dd, k, SD)
            rows = dot(pick(T_DEC_CELL, k, DROWS, CELLS), bgath[...])
            put_rows(bs, k, rows * column(T_DEC_SCALE, k, DROWS) * slope(pre), SD)
            send(2, k, bs, bd, -1)
            own(k, bs, bd)

    loop(back_send)

    def over_lat(src, dst, slot):
        return [
            to(src.at[lax.rem(la + d, 4)], dst.at[d - 1], slot + d, device(d, 0, me))
            for d in (2, 1, 3)
        ]

    def over_lon(src, dst, slot):
        return [
            to(src.at[lax.rem(lo + d, 4)], dst.at[d - 1], slot + d, device(0, d, me))
            for d in (2, 1, 3)
        ]

    scale = 1.0 / CELLS
    grad = (dot_tn(gath[...], bhalf[...]) * scale).astype(BF)
    ga[0] = grad[:, 0:384]
    ga[1, :, 0:128] = grad[:, 384:512]
    ga[1, :, 128:256] = (dot_tn(blend[...], resid[...]) * scale).astype(BF)
    ga[1, :, 256:384] = jnp.zeros((W, 128), BF)
    arrived([to(ga.at[1 - core], la_c, 0, partner)])
    for j in range(4):
        rows = pl.ds(j * 128, 128)
        ha[j] = (ga[core, rows, :].astype(F32) + la_c[rows, :].astype(F32)).astype(BF)
    wait_a = over_lat(ha, la_y, 0)

    acc_n[...] = jnp.zeros_like(acc_n)

    def back_take(k):
        @pl.when(valid(k, 1))
        def _():
            await_bytes(rsem, 2, k, bd)
            rows = get_rows(bd, k, SD).astype(BF)
            acc_n[...] += dot(place(T_DEC_NODE, k, NODES, DROWS).astype(BF), rows)

    loop(back_take)

    back_pre = acc_n[...].astype(BF)
    back_node = dot_nt(back_pre, w_msg[...])
    back_node_half = back_node.astype(BF)
    back_act = (dot_nt(back_node_half, w_down[...]) * slope(act[...])).astype(BF)
    back_norm = dot_nt(back_act, w_up[...]) * node_gain[...]
    state = nstate[...]
    inv_rms = lax.rsqrt(jnp.mean(state * state, axis=-1, keepdims=True) + 1e-05)
    mean_term = jnp.mean(state * back_norm, axis=-1, keepdims=True)
    back_state = back_node + inv_rms * back_norm - state * (inv_rms * inv_rms * inv_rms * mean_term)
    back_half = back_state.astype(BF)
    backw[...] = dot_nt(back_half, w_enc[...]).astype(BF)

    def enc_back_send(k):
        @pl.when(valid(k, -1))
        def _():
            put_rows(fs, k, dot(pick(T_ENC_NODE, k, EROWS, NODES), backw[...]), SEP)
            send(3, k, fs, fd, -1)
            own(k, fs, fd)

    gb[0, :, 0:512] = (dot_tn(nhalf[...], back_pre) * scale).astype(BF)
    gb[0, :, 512:1024] = (dot_tn(hidden[...], back_node_half) * scale).astype(BF)
    gb[1, :, 0:512] = (dot_tn(normed[...], back_act) * scale).astype(BF)
    gb[1, :, 512:1024] = (dot_tn(aggb[...], back_half) * scale).astype(BF)
    wait_b = [to(gb.at[1 - core], lb_c, 4, partner)]

    loop(enc_back_send, 0, 3)

    arrived(wait_b)
    for j in range(4):
        rows = pl.ds(j * 128, 128)
        both = gb[core, rows, :].astype(F32) + lb_c[rows, :].astype(F32)
        hu[j] = both[:, 0:512].astype(BF)
        for i in range(4):
            hv[i, j] = both[i * 32 : (i + 1) * 32, 512:1024].astype(BF)
    wait_u = over_lat(hu, lu_y, 4)
    wait_v = over_lon(hv, lv_z, 8)
    arrived(wait_a)
    total = ha[la].astype(F32) + la_y[0].astype(F32) + la_y[1].astype(F32) + la_y[2].astype(F32)
    for j in range(4):
        ha2[j] = total[j * 32 : (j + 1) * 32, :].astype(BF)
    wait_a = over_lon(ha2, la_z, 12)

    loop(enc_back_send, 3, 6)

    arrived(wait_u)
    total = hu[la].astype(F32) + lu_y[0].astype(F32) + lu_y[1].astype(F32) + lu_y[2].astype(F32)
    for j in range(4):
        hu2[j] = total[j * 32 : (j + 1) * 32, :].astype(BF)
    wait_u = over_lon(hu2, lu_z, 16)
    arrived(wait_v)
    for j in range(4):
        total = hv[lo, j].astype(F32) + lv_z[0, j].astype(F32)
        hv2[j] = (total + lv_z[1, j].astype(F32) + lv_z[2, j].astype(F32)).astype(BF)
    wait_v = over_lat(hv2, lv_y, 20)

    loop(enc_back_send, 6, 9)

    def finished(own_part, landed):
        total = own_part.astype(F32) + landed[0].astype(F32)
        return total + landed[1].astype(F32) + landed[2].astype(F32)

    arrived(wait_u)
    arrived(wait_v)
    arrived(wait_a)
    for at, total in (
        (0, finished(hu2[lo], lu_z)),
        (512, finished(hv2[la], lv_y)),
        (1024, finished(ha2[lo], la_z)),
    ):
        for j in range(8):
            hm[j, :, at : at + total.shape[1]] = total[j * 4 : (j + 1) * 4, :]
    wait_m = []
    for d in (4, 3, 5, 2, 6, 1, 7):
        part = lax.rem(me + d, 8)
        wait_m.append(to(hm.at[part], lm.at[d - 1], 32 + d, device(0, 0, part)))

    def enc_back_take(k):
        @pl.when(valid(k, 1))
        def _():
            await_bytes(rsem, 3, k, fd)
            rows = get_rows(fd, k, SEP).astype(BF)
            weight = table[pl.ds(T_ENC_SCALE + k, 1), :][:, 0:EROWS]
            spread = (place(T_ENC_CELL, k, CELLS, EROWS) * weight).astype(BF)
            grid_grad[...] += dot(spread, rows)

    loop(enc_back_take)

    arrived(wait_m)
    same = hm[me]
    other = lm[0]
    same = same + lm[1] + lm[3] + lm[5]
    other = other + lm[2] + lm[4] + lm[6]
    low = jnp.where(core == 0, same, other)
    high = jnp.where(core == 0, other, same)
    g_msg[...] = low[:, 0:512]
    g_down[...] = low[:, 512:1024]
    g_dec[:, 0:384] = low[:, 1024:1408]
    g_up[...] = high[:, 0:512]
    g_enc[...] = high[:, 512:1024]
    g_dec[:, 384:512] = high[:, 1024:1152]
    g_out[...] = high[:, 1152 : 1152 + 84]

    for c in sent:
        c.wait_send()

    def drain(k):
        @pl.when(valid(k, 1))
        def _():
            await_bytes(ssem, 0, k, es)
            await_bytes(ssem, 1, k, ds_)

        @pl.when(valid(k, -1))
        def _():
            await_bytes(ssem, 2, k, bs)
            await_bytes(ssem, 3, k, fs)

    loop(drain)


def scratch():
    v = pltpu.VMEM
    return [
        v((9, 8, SE), jnp.int32),
        v((9, 8, SE), jnp.int32),
        v((9, 8, SD), jnp.int32),
        v((9, 8, SD), jnp.int32),
        v((9, 8, SE), F32),
        v((9, 8, SD), F32),
        v((9, 1, 8), jnp.int32),
        v((8, 128), F32),
        v((84, CELLS), BF),
        v((84, W), BF),
        v((1, W), F32),
        v((CELLS, W), BF),
        v((NODES, W), BF),
        v((W, W), BF),
        v((W, W), BF),
        v((W, W), BF),
        v((W, W), BF),
        v((W, W), BF),
        v((128, CELLS), F32),
        v((8, 256), F32),
        v((128, 256), F32),
        v((256, 128), F32),
        v((8, 16, 128), F32),
        v((2, 16, 128), F32),
        v((2, NODES, W), BF),
        v((18, SD, W), BF),
        v((NODES, W), BF),
        v((72, SEP, W), BF),
        v((72, SEP, W), BF),
        v((72, SD, W), BF),
        v((72, SD, W), BF),
        v((72, SD, W), BF),
        v((72, SD, W), BF),
        v((72, SEP, W), BF),
        v((72, SEP, W), BF),
        v((NODES, W), F32),
        v((CELLS, W), F32),
        v((CELLS, W), BF),
        v((CELLS, W), BF),
        v((CELLS, W), BF),
        v((CELLS, W), BF),
        v((CELLS, 128), BF),
        v((128, W), BF),
        v((NODES, W), F32),
        v((NODES, W), F32),
        v((NODES, W), BF),
        v((NODES, W), BF),
        v((NODES, W), BF),
        v((NODES, W), BF),
        v((NODES, W), BF),
        v((2, W, 384), BF),
        v((W, 384), BF),
        v((4, 128, 384), BF),
        v((3, 128, 384), BF),
        v((4, 32, 384), BF),
        v((3, 32, 384), BF),
        v((2, W, 1024), BF),
        v((W, 1024), BF),
        v((4, 128, 512), BF),
        v((3, 128, 512), BF),
        v((4, 32, 512), BF),
        v((3, 32, 512), BF),
        v((4, 4, 32, 512), BF),
        v((3, 4, 32, 512), BF),
        v((4, 32, 512), BF),
        v((3, 32, 512), BF),
        v((8, 4, 1408), F32),
        v((7, 4, 1408), F32),
        pltpu.SemaphoreType.DMA((4, 9)),
        pltpu.SemaphoreType.DMA((4, 9)),
        pltpu.SemaphoreType.DMA((40,)),
        pltpu.SemaphoreType.DMA((40,)),
        pltpu.SemaphoreType.DMA((18,)),
    ]


def on_device(
    grid_latent,
    target,
    area,
    mesh_latent,
    node_gain,
    w_enc,
    w_up,
    w_down,
    w_msg,
    w_dec,
    w_out,
    enc_cell,
    enc_live,
    enc_weight,
    enc_node,
    dec_node,
    dec_cell,
    dec_weight,
):
    vm = pl.BlockSpec(memory_space=pltpu.VMEM)
    small = jax.ShapeDtypeStruct((4, W), F32)
    any_space = pl.BlockSpec(memory_space=pl.ANY)
    shapes = (jax.ShapeDtypeStruct((CELLS, W), F32),) + (small,) * 5
    shapes += (jax.ShapeDtypeStruct((4, 84), F32),)
    outs = pl.pallas_call(
        kernel,
        out_shape=shapes,
        in_specs=[any_space] * 18,
        out_specs=(vm,) * 7,
        scratch_shapes=scratch(),
        compiler_params=pltpu.CompilerParams(
            collective_id=0, has_side_effects=True, vmem_limit_bytes=VMEM_LIMIT
        ),
        name="step",
    )(
        enc_cell.reshape(9, 8, SE),
        enc_node.reshape(9, 8, SE),
        dec_node.reshape(9, 8, SD),
        dec_cell.reshape(9, 8, SD),
        enc_weight.reshape(9, 8, SE),
        dec_weight.reshape(9, 8, SD),
        enc_live.reshape(9, 1, 8),
        area.reshape(8, 128),
        target.T,
        w_out.T,
        node_gain.reshape(1, W),
        grid_latent,
        mesh_latent,
        w_enc,
        w_up,
        w_down,
        w_msg,
        w_dec,
    )
    return pl.pallas_call(
        finish,
        out_shape=shapes,
        in_specs=[any_space] * 7,
        out_specs=(any_space,) * 7,
        scratch_shapes=[
            pltpu.VMEM((CELLS, W), F32),
            pltpu.VMEM((5, 4, W), F32),
            pltpu.VMEM((4, 84), F32),
            pltpu.SemaphoreType.DMA((10,)),
            pltpu.SemaphoreType.DMA((10,)),
        ],
        compiler_params=pltpu.CompilerParams(vmem_limit_bytes=VMEM_LIMIT),
        name="finish",
    )(*outs)


def finish(*refs):
    grid, small, head, arrive, leave = refs[14:]
    parts = [
        (refs[0].at[rows], grid.at[rows], refs[7].at[rows])
        for rows in (pl.ds(b * 256, 256) for b in range(4))
    ]
    parts += [(refs[i], small.at[i - 1], refs[7 + i]) for i in range(1, 6)]
    parts.append((refs[6], head, refs[13]))
    inward = [pltpu.make_async_copy(a, b, arrive.at[i]) for i, (a, b, c) in enumerate(parts)]
    outward = [pltpu.make_async_copy(b, c, leave.at[i]) for i, (a, b, c) in enumerate(parts)]
    for copy in inward:
        copy.start()
    for first, second in zip(inward, outward):
        first.wait()
        second.start()
    for copy in outward:
        copy.wait()


def solution(mesh):
    rows = P(AXES, None)
    slots = P(AXES, None, None, None, None)
    in_specs = (
        rows,
        rows,
        P(AXES),
        rows,
        P(),
        P(),
        P(),
        P(),
        P(),
        P(),
        P(),
        slots,
        P(AXES, None, None, None),
        slots,
        slots,
        slots,
        slots,
        slots,
    )
    return jax.shard_map(
        on_device, mesh=mesh, in_specs=in_specs, out_specs=(rows,) * 7, check_vma=False
    )
```

```python
import jax
import jax.numpy as jnp
from jax import lax
from jax.experimental import pallas as pl
from jax.experimental.pallas import tpu as pltpu
from jax.sharding import PartitionSpec as P

AXES = ("lat", "lon", "mesh")
MESH_ID = pl.DeviceIdType.MESH
W = 512
CELLS = 1024
NODES = 320
SE = 21
SEP = 24
SD = 32
EROWS = 8 * SEP
DROWS = 8 * SD
T_ENC_CELL, T_ENC_NODE, T_DEC_NODE, T_DEC_CELL, T_ENC_SCALE, T_DEC_SCALE, T_AREA = (
    0,
    9,
    18,
    27,
    36,
    45,
    54,
)
VMEM_LIMIT = 67043328
BF = jnp.bfloat16
F32 = jnp.float32


def dot(a, b):
    return jnp.dot(a, b, preferred_element_type=F32)


def dot_nt(a, b):
    return lax.dot_general(a, b, (((1,), (1,)), ((), ())), preferred_element_type=F32)


def dot_tn(a, b):
    return lax.dot_general(a, b, (((0,), (0,)), ((), ())), preferred_element_type=F32)


def sigmoid(x):
    return 0.5 * jnp.tanh(0.5 * x) + 0.5


def slope(x):
    s = sigmoid(x)
    return s * (1.0 + x * (1.0 - s))


def kernel(
    enc_cell_in,
    enc_node_in,
    dec_node_in,
    dec_cell_in,
    enc_weight_in,
    dec_weight_in,
    enc_live_in,
    area_in,
    target_t_in,
    w_out_t_in,
    node_gain_in,
    grid_latent_in,
    mesh_latent_in,
    w_enc_in,
    w_up_in,
    w_down_in,
    w_msg_in,
    w_dec_in,
    grid_out,
    g_enc,
    g_up,
    g_down,
    g_msg,
    g_dec,
    g_out,
    enc_cell,
    enc_node,
    dec_node,
    dec_cell,
    enc_weight,
    dec_weight,
    enc_live,
    area,
    target_t,
    w_out_t,
    node_gain,
    grid_latent,
    mesh_latent,
    w_enc,
    w_up,
    w_down,
    w_msg,
    w_dec,
    target,
    pad,
    table,
    cols,
    grid_grad,
    grid_half,
    os_,
    by_part,
    far_part,
    far_rows,
    far_out,
    backw,
    es,
    ed,
    ds_,
    dd,
    bs,
    bd,
    fs,
    fd,
    acc_n,
    acc_c,
    gath,
    blend,
    bhalf,
    bgath,
    resid,
    wo,
    nstate,
    act,
    normed,
    hidden,
    nhalf,
    prew,
    aggb,
    ga,
    la_c,
    ha,
    la_y,
    ha2,
    la_z,
    gb,
    lb_c,
    hu,
    lu_y,
    hu2,
    lu_z,
    hv,
    lv_z,
    hv2,
    lv_y,
    hm,
    lm,
    ssem,
    rsem,
    gs,
    gr,
    ls,
):
    la, lo, me = lax.axis_index("lat"), lax.axis_index("lon"), lax.axis_index("mesh")
    core = lax.rem(me, 2)
    far_same = lax.rem(me + 4, 8)
    far_other = far_same + 1 - 2 * core

    def device(dla, dlo, part):
        return {"lat": lax.rem(la + dla, 4), "lon": lax.rem(lo + dlo, 4), "mesh": part}

    barrier = pltpu.get_barrier_semaphore()
    peers = 0
    for p in range(3):
        for q in range(3):
            for d in range(8):
                if p == 1 and q == 1 and d == 0:
                    continue
                pl.semaphore_signal(
                    barrier,
                    inc=1,
                    device_id=device(p + 3, q + 3, lax.rem(me + d, 8)),
                    device_id_type=MESH_ID,
                )
                peers += 1
    for dla, dlo in ((2, 0), (0, 2)):
        pl.semaphore_signal(
            barrier, inc=1, device_id=device(dla, dlo, me), device_id_type=MESH_ID
        )
        peers += 1

    loads = []
    for i, (src, dst) in enumerate(
        (
            (enc_cell_in, enc_cell),
            (enc_node_in, enc_node),
            (dec_node_in, dec_node),
            (dec_cell_in, dec_cell),
            (enc_weight_in, enc_weight),
            (dec_weight_in, dec_weight),
            (enc_live_in, enc_live),
            (area_in, area),
            (target_t_in, target_t),
            (w_out_t_in, w_out_t),
            (node_gain_in, node_gain),
            (grid_latent_in, grid_latent),
            (mesh_latent_in, mesh_latent),
            (w_enc_in, w_enc),
            (w_up_in, w_up),
            (w_down_in, w_down),
            (w_msg_in, w_msg),
            (w_dec_in, w_dec),
        )
    ):
        loads.append(pltpu.make_async_copy(src, dst, ls.at[i]))
        loads[i].start()

    for copy in loads[:11]:
        copy.wait()

    table[...] = jnp.zeros_like(table)
    pad[...] = jnp.zeros_like(pad)

    def fill(k, carry):
        def put(block, value, slots, stride):
            pad[:, 0:slots] = value
            row = pad[0:1, :]
            for m in range(1, 8):
                row = row + pltpu.roll(pad[m : m + 1, :], m * stride, axis=1)
            table[pl.ds(block + k, 1), :] = row

        put(T_DEC_NODE, dec_node[k].astype(F32), SD, SD)
        for m in range(8):
            by_part[m, pl.ds(k, 1), :] = pad[m : m + 1, 0:128]
        put(T_DEC_CELL, dec_cell[k].astype(F32), SD, SD)
        put(T_DEC_SCALE, dec_weight[k], SD, SD)
        pad[...] = jnp.zeros_like(pad)
        put(T_ENC_CELL, enc_cell[k].astype(F32), SE, SEP)
        put(T_ENC_NODE, enc_node[k].astype(F32), SE, SEP)
        here = lax.broadcasted_iota(jnp.int32, (8, 8), 0) == lax.broadcasted_iota(
            jnp.int32, (8, 8), 1
        )
        live = jnp.sum(jnp.where(here, enc_live[k].astype(F32), 0.0), axis=1, keepdims=True)
        slot = lax.broadcasted_iota(jnp.int32, (8, SE), 1).astype(F32)
        put(T_ENC_SCALE, jnp.where(slot < live, enc_weight[k], 0.0), SE, SEP)
        return carry

    lax.fori_loop(0, 9, fill, 0)
    for b in range(4):
        table[T_AREA + b : T_AREA + b + 1, 0:128] = area[2 * b : 2 * b + 1, :]
        table[T_AREA + b : T_AREA + b + 1, 128:256] = area[2 * b + 1 : 2 * b + 2, :]
    cols[...] = table[...].T
    wo[...] = jnp.zeros_like(wo)
    wo[0:84, :] = w_out_t[...]
    target[...] = jnp.zeros_like(target)
    target[0:84, :] = target_t[...].astype(F32)
    loads[11].wait()

    def column(block, k, rows):
        turned = pltpu.roll(cols[...], lax.rem(128 - (block + k), 128), axis=1)
        return turned[0:rows, 0:1]

    def pick(block, k, rows, width):
        index = column(block, k, rows).astype(jnp.int32)
        return (index == lax.broadcasted_iota(jnp.int32, (rows, width), 1)).astype(F32).astype(BF)

    def place(block, k, rows, width):
        index = table[pl.ds(block + k, 1), :][:, 0:width].astype(jnp.int32)
        return (index == lax.broadcasted_iota(jnp.int32, (rows, width), 0)).astype(F32)

    def chunk_of(t):
        return lax.rem(4 * t + 8, 9)

    def valid(k, sign):
        at = la + sign * (k // 3 - 1)
        return (at >= 0) & (at < 4)

    def to(src, dst, slot, where):
        copy = pltpu.make_async_remote_copy(
            src_ref=src,
            dst_ref=dst,
            send_sem=gs.at[slot],
            recv_sem=gr.at[slot],
            device_id=where,
            device_id_type=MESH_ID,
        )
        copy.start()
        sent.append(copy)
        return copy

    def arrived(copies):
        for copy in copies:
            copy.wait_recv()

    sent = []
    partner = device(0, 0, me + 1 - 2 * core)

    def send(phase, k, src, dst, sign):
        dla = k // 3 - 1
        dlo = lax.rem(k, 3) - 1
        for d in (4, 3, 5, 2, 6, 1, 7, 0):
            if phase == 1 and d in (3, 4, 5):
                continue
            part = lax.rem(me + d, 8)
            copy = pltpu.make_async_remote_copy(
                src_ref=src.at[k * 8 + part],
                dst_ref=dst.at[k * 8 + me],
                send_sem=ssem.at[phase, k],
                recv_sem=rsem.at[phase, k],
                device_id=device(sign * dla + 4, sign * dlo + 4, part),
                device_id_type=MESH_ID,
            )
            if d == 0:
                pl.when(k != 4)(copy.start)
            else:
                copy.start()
        if phase == 1:
            part = lax.rem(me + 3 + 2 * core, 8)
            pltpu.make_async_remote_copy(
                src_ref=src.at[k * 8 + part],
                dst_ref=dst.at[k * 8 + me],
                send_sem=ssem.at[phase, k],
                recv_sem=rsem.at[phase, k],
                device_id=device(sign * dla + 4, sign * dlo + 4, part),
                device_id_type=MESH_ID,
            ).start()

    def await_bytes(sem, phase, k, buf):
        whole = buf.at[pl.ds(k * 8, 8)]
        most = buf.at[pl.ds(k * 8, 5 if phase == 1 else 7)]

        @pl.when(k != 4)
        def _():
            pltpu.make_async_copy(whole, whole, sem.at[phase, k]).wait()

        @pl.when(k == 4)
        def _():
            pltpu.make_async_copy(most, most, sem.at[phase, k]).wait()

    def own(k, src, dst):
        @pl.when(k == 4)
        def _():
            dst[4 * 8 + me] = src[4 * 8 + me]

    def put_rows(buf, k, rows_f32, slots):
        for m in range(8):
            buf[k * 8 + m] = rows_f32[m * slots : (m + 1) * slots, :].astype(BF)

    def get_rows(buf, k, slots):
        return buf[pl.ds(k * 8, 8)].astype(F32).reshape(8 * slots, W)

    def loop(body, first=0, last=9):
        def step(t, carry):
            body(chunk_of(t))
            return carry

        lax.fori_loop(first, last, step, 0)

    def enc_make(k):
        @pl.when(valid(k, 1))
        def _():
            rows = dot(pick(T_ENC_CELL, k, EROWS, CELLS), grid_latent[...])
            put_rows(es, k, rows * column(T_ENC_SCALE, k, EROWS), SEP)

    loop(enc_make, 0, 3)
    pl.semaphore_wait(barrier, peers)

    def enc_send(k):
        @pl.when(valid(k, 1))
        def _():
            send(0, k, es, ed, 1)
            own(k, es, ed)

    def enc_both(k):
        enc_make(k)
        enc_send(k)

    loop(enc_send, 0, 3)
    far_tables = [
        to(by_part.at[far_same], far_part.at[0], 27, device(0, 0, far_same)),
        to(by_part.at[far_other], far_part.at[1], 28, device(0, 0, far_other)),
    ]
    loop(enc_both, 3, 9)

    acc_n[...] = jnp.zeros_like(acc_n)

    def enc_take(k):
        @pl.when(valid(k, -1))
        def _():
            await_bytes(rsem, 0, k, ed)
            rows = get_rows(ed, k, SEP).astype(BF)
            acc_n[...] += dot(place(T_ENC_NODE, k, NODES, EROWS).astype(BF), rows)

    loop(enc_take)

    for copy in loads[12:]:
        copy.wait()
    aggb[...] = acc_n[...].astype(BF)
    state = mesh_latent[...].astype(F32) + dot(aggb[...], w_enc[...])
    nstate[...] = state
    inv_rms = lax.rsqrt(jnp.mean(state * state, axis=-1, keepdims=True) + 1e-05)
    normed[...] = (state * inv_rms * node_gain[...]).astype(BF)
    activation = dot(normed[...], w_up[...])
    act[...] = activation
    hidden[...] = (activation * sigmoid(activation)).astype(BF)
    nhalf[...] = (nstate[...] + dot(hidden[...], w_down[...])).astype(BF)
    prew[...] = dot(nhalf[...], w_msg[...]).astype(BF)

    def dec_send(k):
        @pl.when(valid(k, 1))
        def _():
            put_rows(ds_, k, dot(pick(T_DEC_NODE, k, DROWS, NODES), prew[...]), SD)
            send(1, k, ds_, dd, 1)
            own(k, ds_, dd)

    far_block = to(prew, far_rows.at[0], 29, device(0, 0, far_same))
    loop(dec_send)

    def relay(i, source):
        turned = far_part[i].T
        index = jnp.concatenate([turned[0:SD, k : k + 1] for k in range(9)], axis=0)
        width = lax.broadcasted_iota(jnp.int32, (9 * SD, NODES), 1)
        chosen = (index.astype(jnp.int32) == width).astype(F32).astype(BF)
        rows = dot(chosen, far_rows[i]).astype(BF)
        for k in range(9):
            far_out[i * 9 + k] = rows[k * SD : (k + 1) * SD, :]

        def relay_send(k):
            @pl.when(valid(k, 1) & (k != 4))
            def _():
                pltpu.make_async_remote_copy(
                    src_ref=far_out.at[i * 9 + k],
                    dst_ref=dd.at[k * 8 + source],
                    send_sem=ssem.at[1, k],
                    recv_sem=rsem.at[1, k],
                    device_id=device(k // 3 + 3, lax.rem(k, 3) + 3, me),
                    device_id_type=MESH_ID,
                ).start()

        loop(relay_send)
        dd[4 * 8 + source] = far_out[i * 9 + 4]

    arrived(far_tables)
    arrived([far_block])
    far_block = to(far_rows.at[0], far_rows.at[1], 30, partner)
    relay(0, far_same)
    arrived([far_block])
    relay(1, far_other)
    acc_c[...] = jnp.zeros_like(acc_c)

    def dec_take(k):
        @pl.when(valid(k, -1))
        def _():
            await_bytes(rsem, 1, k, dd)
            pre = get_rows(dd, k, SD)
            rows = (column(T_DEC_SCALE, k, DROWS) * (pre * sigmoid(pre))).astype(BF)
            acc_c[...] += dot(place(T_DEC_CELL, k, CELLS, DROWS).astype(BF), rows)

    loop(dec_take)

    for b in range(4):
        at = pl.ds(b * 256, 256)
        gathered = acc_c[at, :].astype(BF)
        gath[at, :] = gathered
        blended = (grid_latent[at, :].astype(F32) + dot(gathered, w_dec[...])).astype(BF)
        blend[at, :] = blended
        output = dot_nt(blended, wo[...])
        weight = cols[0:256, T_AREA + b : T_AREA + b + 1]
        residual = (weight * (output - target[:, at].T)).astype(BF)
        resid[at, :] = residual
        back = dot(residual, wo[...])
        grid_grad[at, :] = back
        half = back.astype(BF)
        bhalf[at, :] = half
        bgath[at, :] = dot_nt(half, w_dec[...]).astype(BF)

    def back_send(k):
        @pl.when(valid(k, -1))
        def _():
            pre = get_rows(dd, k, SD)
            rows = dot(pick(T_DEC_CELL, k, DROWS, CELLS), bgath[...])
            put_rows(bs, k, rows * column(T_DEC_SCALE, k, DROWS) * slope(pre), SD)
            send(2, k, bs, bd, -1)
            own(k, bs, bd)

    loop(back_send)

    def over_lat(src, dst, slot):
        return [
            to(src.at[lax.rem(la + d, 4)], dst.at[d - 1], slot + d, device(d, 0, me))
            for d in (2, 1, 3)
        ]

    def over_lon(src, dst, slot):
        return [
            to(src.at[lax.rem(lo + d, 4)], dst.at[d - 1], slot + d, device(0, d, me))
            for d in (2, 1, 3)
        ]

    scale = 1.0 / CELLS
    grad = (dot_tn(gath[...], bhalf[...]) * scale).astype(BF)
    ga[0] = grad[:, 0:384]
    ga[1, :, 0:128] = grad[:, 384:512]
    ga[1, :, 128:256] = (dot_tn(blend[...], resid[...]) * scale).astype(BF)
    ga[1, :, 256:384] = jnp.zeros((W, 128), BF)
    arrived([to(ga.at[1 - core], la_c, 0, partner)])
    for j in range(4):
        rows = pl.ds(j * 128, 128)
        ha[j] = (ga[core, rows, :].astype(F32) + la_c[rows, :].astype(F32)).astype(BF)
    wait_a = over_lat(ha, la_y, 0)

    acc_n[...] = jnp.zeros_like(acc_n)

    def back_take(k):
        @pl.when(valid(k, 1))
        def _():
            await_bytes(rsem, 2, k, bd)
            rows = get_rows(bd, k, SD).astype(BF)
            acc_n[...] += dot(place(T_DEC_NODE, k, NODES, DROWS).astype(BF), rows)

    loop(back_take)

    back_pre = acc_n[...].astype(BF)
    back_node = dot_nt(back_pre, w_msg[...])
    back_node_half = back_node.astype(BF)
    back_act = (dot_nt(back_node_half, w_down[...]) * slope(act[...])).astype(BF)
    back_norm = dot_nt(back_act, w_up[...]) * node_gain[...]
    state = nstate[...]
    inv_rms = lax.rsqrt(jnp.mean(state * state, axis=-1, keepdims=True) + 1e-05)
    mean_term = jnp.mean(state * back_norm, axis=-1, keepdims=True)
    back_state = back_node + inv_rms * back_norm - state * (inv_rms * inv_rms * inv_rms * mean_term)
    back_half = back_state.astype(BF)
    backw[...] = dot_nt(back_half, w_enc[...]).astype(BF)

    def enc_back_send(k):
        @pl.when(valid(k, -1))
        def _():
            put_rows(fs, k, dot(pick(T_ENC_NODE, k, EROWS, NODES), backw[...]), SEP)
            send(3, k, fs, fd, -1)
            own(k, fs, fd)

    loop(enc_back_send, 0, 5)

    gb[0, :, 0:512] = (dot_tn(nhalf[...], back_pre) * scale).astype(BF)
    gb[0, :, 512:1024] = (dot_tn(hidden[...], back_node_half) * scale).astype(BF)
    gb[1, :, 0:512] = (dot_tn(normed[...], back_act) * scale).astype(BF)
    gb[1, :, 512:1024] = (dot_tn(aggb[...], back_half) * scale).astype(BF)
    wait_b = [to(gb.at[1 - core], lb_c, 4, partner)]
    loop(enc_back_send, 5, 9)

    arrived(wait_b)
    for j in range(4):
        rows = pl.ds(j * 128, 128)
        both = gb[core, rows, :].astype(F32) + lb_c[rows, :].astype(F32)
        hu[j] = both[:, 0:512].astype(BF)
        for i in range(4):
            hv[i, j] = both[i * 32 : (i + 1) * 32, 512:1024].astype(BF)
    wait_u = over_lat(hu, lu_y, 4)
    wait_v = over_lon(hv, lv_z, 8)
    arrived(wait_a)
    total = ha[la].astype(F32) + la_y[0].astype(F32) + la_y[1].astype(F32) + la_y[2].astype(F32)
    for j in range(4):
        ha2[j] = total[j * 32 : (j + 1) * 32, :].astype(BF)
    wait_a = over_lon(ha2, la_z, 12)

    arrived(wait_u)
    total = hu[la].astype(F32) + lu_y[0].astype(F32) + lu_y[1].astype(F32) + lu_y[2].astype(F32)
    for j in range(4):
        hu2[j] = total[j * 32 : (j + 1) * 32, :].astype(BF)
    wait_u = over_lon(hu2, lu_z, 16)
    arrived(wait_v)
    for j in range(4):
        total = hv[lo, j].astype(F32) + lv_z[0, j].astype(F32)
        hv2[j] = (total + lv_z[1, j].astype(F32) + lv_z[2, j].astype(F32)).astype(BF)
    wait_v = over_lat(hv2, lv_y, 20)

    def finished(own_part, landed):
        total = own_part.astype(F32) + landed[0].astype(F32)
        return total + landed[1].astype(F32) + landed[2].astype(F32)

    arrived(wait_u)
    arrived(wait_v)
    arrived(wait_a)
    for at, total in (
        (0, finished(hu2[lo], lu_z)),
        (512, finished(hv2[la], lv_y)),
        (1024, finished(ha2[lo], la_z)),
    ):
        for j in range(8):
            hm[j, :, at : at + total.shape[1]] = total[j * 4 : (j + 1) * 4, :].astype(BF)
    wait_m = []
    for d in (4, 3, 5, 2, 6, 1, 7):
        part = lax.rem(me + d, 8)
        wait_m.append(to(hm.at[part], lm.at[d - 1], 32 + d, device(0, 0, part)))

    def enc_back_take(k):
        @pl.when(valid(k, 1))
        def _():
            await_bytes(rsem, 3, k, fd)
            rows = get_rows(fd, k, SEP).astype(BF)
            weight = table[pl.ds(T_ENC_SCALE + k, 1), :][:, 0:EROWS]
            spread = (place(T_ENC_CELL, k, CELLS, EROWS) * weight).astype(BF)
            grid_grad[...] += dot(spread, rows)

    loop(enc_back_take, 0, 8)

    await_bytes(rsem, 3, 4, fd)
    rows = get_rows(fd, 4, SEP).astype(BF)
    weight = table[T_ENC_SCALE + 4 : T_ENC_SCALE + 5, 0:EROWS]
    index = table[T_ENC_CELL + 4 : T_ENC_CELL + 5, 0:EROWS].astype(jnp.int32)
    leave = []
    for b in range(4):
        at = pl.ds(b * 256, 256)
        here = index == lax.broadcasted_iota(jnp.int32, (256, EROWS), 0) + b * 256
        spread = (here.astype(F32) * weight).astype(BF)
        grid_half[at, :] = (grid_grad[at, :] + dot(spread, rows)).astype(BF)
        leave.append(pltpu.make_async_copy(grid_half.at[at], grid_out.at[at], os_.at[b]))
        leave[b].start()

    arrived(wait_m)
    landed = [lm[d].astype(F32) for d in range(7)]
    same = hm[me].astype(F32)
    other = landed[0]
    same = same + landed[1] + landed[3] + landed[5]
    other = other + landed[2] + landed[4] + landed[6]
    low = jnp.where(core == 0, same, other)
    high = jnp.where(core == 0, other, same)
    g_msg[...] = low[:, 0:512]
    g_down[...] = low[:, 512:1024]
    g_dec[:, 0:384] = low[:, 1024:1408]
    g_up[...] = high[:, 0:512]
    g_enc[...] = high[:, 512:1024]
    g_dec[:, 384:512] = high[:, 1024:1152]
    g_out[...] = high[:, 1152 : 1152 + 84]

    for c in sent:
        c.wait_send()
    for c in leave:
        c.wait()

    def drain(k):
        @pl.when(valid(k, 1))
        def _():
            await_bytes(ssem, 0, k, es)
            await_bytes(ssem, 1, k, ds_)

        @pl.when(valid(k, -1))
        def _():
            await_bytes(ssem, 2, k, bs)
            await_bytes(ssem, 3, k, fs)

    loop(drain)


def scratch():
    v = pltpu.VMEM
    return [
        v((9, 8, SE), jnp.int32),
        v((9, 8, SE), jnp.int32),
        v((9, 8, SD), jnp.int32),
        v((9, 8, SD), jnp.int32),
        v((9, 8, SE), F32),
        v((9, 8, SD), F32),
        v((9, 1, 8), jnp.int32),
        v((8, 128), F32),
        v((84, CELLS), BF),
        v((84, W), BF),
        v((1, W), F32),
        v((CELLS, W), BF),
        v((NODES, W), BF),
        v((W, W), BF),
        v((W, W), BF),
        v((W, W), BF),
        v((W, W), BF),
        v((W, W), BF),
        v((128, CELLS), F32),
        v((8, 256), F32),
        v((128, 256), F32),
        v((256, 128), F32),
        v((CELLS, W), F32),
        v((CELLS, W), BF),
        pltpu.SemaphoreType.DMA((4,)),
        v((8, 16, 128), F32),
        v((2, 16, 128), F32),
        v((2, NODES, W), BF),
        v((18, SD, W), BF),
        v((NODES, W), BF),
        v((72, SEP, W), BF),
        v((72, SEP, W), BF),
        v((72, SD, W), BF),
        v((72, SD, W), BF),
        v((72, SD, W), BF),
        v((72, SD, W), BF),
        v((72, SEP, W), BF),
        v((72, SEP, W), BF),
        v((NODES, W), F32),
        v((CELLS, W), F32),
        v((CELLS, W), BF),
        v((CELLS, W), BF),
        v((CELLS, W), BF),
        v((CELLS, W), BF),
        v((CELLS, 128), BF),
        v((128, W), BF),
        v((NODES, W), F32),
        v((NODES, W), F32),
        v((NODES, W), BF),
        v((NODES, W), BF),
        v((NODES, W), BF),
        v((NODES, W), BF),
        v((NODES, W), BF),
        v((2, W, 384), BF),
        v((W, 384), BF),
        v((4, 128, 384), BF),
        v((3, 128, 384), BF),
        v((4, 32, 384), BF),
        v((3, 32, 384), BF),
        v((2, W, 1024), BF),
        v((W, 1024), BF),
        v((4, 128, 512), BF),
        v((3, 128, 512), BF),
        v((4, 32, 512), BF),
        v((3, 32, 512), BF),
        v((4, 4, 32, 512), BF),
        v((3, 4, 32, 512), BF),
        v((4, 32, 512), BF),
        v((3, 32, 512), BF),
        v((8, 4, 1408), BF),
        v((7, 4, 1408), BF),
        pltpu.SemaphoreType.DMA((4, 9)),
        pltpu.SemaphoreType.DMA((4, 9)),
        pltpu.SemaphoreType.DMA((40,)),
        pltpu.SemaphoreType.DMA((40,)),
        pltpu.SemaphoreType.DMA((18,)),
    ]


def on_device(
    grid_latent,
    target,
    area,
    mesh_latent,
    node_gain,
    w_enc,
    w_up,
    w_down,
    w_msg,
    w_dec,
    w_out,
    enc_cell,
    enc_live,
    enc_weight,
    enc_node,
    dec_node,
    dec_cell,
    dec_weight,
):
    vm = pl.BlockSpec(memory_space=pltpu.VMEM)
    small = jax.ShapeDtypeStruct((4, W), F32)
    any_space = pl.BlockSpec(memory_space=pl.ANY)
    rest = (small,) * 5 + (jax.ShapeDtypeStruct((4, 84), F32),)
    outs = pl.pallas_call(
        kernel,
        out_shape=(jax.ShapeDtypeStruct((CELLS, W), BF),) + rest,
        in_specs=[any_space] * 18,
        out_specs=(any_space,) + (vm,) * 6,
        scratch_shapes=scratch(),
        compiler_params=pltpu.CompilerParams(
            collective_id=0, has_side_effects=True, vmem_limit_bytes=VMEM_LIMIT
        ),
        name="step",
    )(
        enc_cell.reshape(9, 8, SE),
        enc_node.reshape(9, 8, SE),
        dec_node.reshape(9, 8, SD),
        dec_cell.reshape(9, 8, SD),
        enc_weight.reshape(9, 8, SE),
        dec_weight.reshape(9, 8, SD),
        enc_live.reshape(9, 1, 8),
        area.reshape(8, 128),
        target.T,
        w_out.T,
        node_gain.reshape(1, W),
        grid_latent,
        mesh_latent,
        w_enc,
        w_up,
        w_down,
        w_msg,
        w_dec,
    )
    return pl.pallas_call(
        finish,
        out_shape=(jax.ShapeDtypeStruct((CELLS, W), F32),) + rest,
        in_specs=[any_space] * 7,
        out_specs=(any_space,) * 7,
        scratch_shapes=[
            pltpu.VMEM((CELLS, W), BF),
            pltpu.VMEM((CELLS, W), F32),
            pltpu.VMEM((5, 4, W), F32),
            pltpu.VMEM((4, 84), F32),
            pltpu.SemaphoreType.DMA((10,)),
            pltpu.SemaphoreType.DMA((10,)),
        ],
        compiler_params=pltpu.CompilerParams(vmem_limit_bytes=VMEM_LIMIT),
        name="finish",
    )(*outs)


def finish(*refs):
    half, full, small, head, arrive, leave = refs[14:]
    blocks = [pl.ds(b * 256, 256) for b in range(4)]
    inward = [(refs[0].at[rows], half.at[rows]) for rows in blocks]
    inward += [(refs[i], small.at[i - 1]) for i in range(1, 6)] + [(refs[6], head)]
    outward = [(full.at[rows], refs[7].at[rows]) for rows in blocks]
    outward += [(small.at[i - 1], refs[7 + i]) for i in range(1, 6)] + [(head, refs[13])]
    inward = [pltpu.make_async_copy(a, b, arrive.at[i]) for i, (a, b) in enumerate(inward)]
    outward = [pltpu.make_async_copy(a, b, leave.at[i]) for i, (a, b) in enumerate(outward)]
    for copy in inward:
        copy.start()
    for i in range(10):
        inward[i].wait()
        if i < 4:
            full[blocks[i], :] = half[blocks[i], :].astype(F32)
        outward[i].start()
    for copy in outward:
        copy.wait()


def solution(mesh):
    rows = P(AXES, None)
    slots = P(AXES, None, None, None, None)
    in_specs = (
        rows,
        rows,
        P(AXES),
        rows,
        P(),
        P(),
        P(),
        P(),
        P(),
        P(),
        P(),
        slots,
        P(AXES, None, None, None),
        slots,
        slots,
        slots,
        slots,
        slots,
    )
    return jax.shard_map(
        on_device, mesh=mesh, in_specs=in_specs, out_specs=(rows,) * 7, check_vma=False
    )
```

```python
import jax
import jax.numpy as jnp
from jax import lax
from jax.experimental import pallas as pl
from jax.experimental.pallas import tpu as pltpu
from jax.sharding import PartitionSpec as P

AXES = ("lat", "lon", "mesh")
MESH_ID = pl.DeviceIdType.MESH
W = 512
CELLS = 1024
NODES = 320
SE = 21
SEP = 24
SD = 32
EROWS = 8 * SEP
DROWS = 8 * SD
T_ENC_CELL, T_ENC_NODE, T_DEC_NODE, T_DEC_CELL, T_ENC_SCALE, T_DEC_SCALE, T_AREA = (
    0,
    9,
    18,
    27,
    36,
    45,
    54,
)
VMEM_LIMIT = 67043328
BF = jnp.bfloat16
F32 = jnp.float32


def dot(a, b):
    return jnp.dot(a, b, preferred_element_type=F32)


def dot_nt(a, b):
    return lax.dot_general(a, b, (((1,), (1,)), ((), ())), preferred_element_type=F32)


def dot_tn(a, b):
    return lax.dot_general(a, b, (((0,), (0,)), ((), ())), preferred_element_type=F32)


def sigmoid(x):
    return 0.5 * jnp.tanh(0.5 * x) + 0.5


def slope(x):
    s = sigmoid(x)
    return s * (1.0 + x * (1.0 - s))


def kernel(
    enc_cell_in,
    enc_node_in,
    dec_node_in,
    dec_cell_in,
    enc_weight_in,
    dec_weight_in,
    enc_live_in,
    area_in,
    target_t_in,
    w_out_t_in,
    node_gain_in,
    grid_latent_in,
    mesh_latent_in,
    w_enc_in,
    w_up_in,
    w_down_in,
    w_msg_in,
    w_dec_in,
    grid_out,
    g_enc,
    g_up,
    g_down,
    g_msg,
    g_dec,
    g_out,
    enc_cell,
    enc_node,
    dec_node,
    dec_cell,
    enc_weight,
    dec_weight,
    enc_live,
    area,
    target_t,
    w_out_t,
    node_gain,
    grid_latent,
    mesh_latent,
    w_enc,
    w_up,
    w_down,
    w_msg,
    w_dec,
    target,
    pad,
    table,
    cols,
    grid_grad,
    grid_half,
    os_,
    by_part,
    far_part,
    far_rows,
    far_out,
    backw,
    kept,
    far_in,
    part_other,
    part_in,
    part_out,
    far_back,
    fsem,
    es,
    ed,
    ds_,
    dd,
    bs,
    bd,
    fs,
    fd,
    acc_n,
    acc_c,
    gath,
    blend,
    bhalf,
    bgath,
    resid,
    wo,
    nstate,
    act,
    normed,
    hidden,
    nhalf,
    prew,
    aggb,
    ga,
    la_c,
    ha,
    la_y,
    ha2,
    la_z,
    gb,
    lb_c,
    hu,
    lu_y,
    hu2,
    lu_z,
    hv,
    lv_z,
    hv2,
    lv_y,
    hm,
    lm,
    ssem,
    rsem,
    gs,
    gr,
    ls,
):
    la, lo, me = lax.axis_index("lat"), lax.axis_index("lon"), lax.axis_index("mesh")
    core = lax.rem(me, 2)
    far_same = lax.rem(me + 4, 8)
    far_other = far_same + 1 - 2 * core

    def device(dla, dlo, part):
        return {"lat": lax.rem(la + dla, 4), "lon": lax.rem(lo + dlo, 4), "mesh": part}

    barrier = pltpu.get_barrier_semaphore()
    peers = 0
    for p in range(3):
        for q in range(3):
            for d in range(8):
                if p == 1 and q == 1 and d == 0:
                    continue
                pl.semaphore_signal(
                    barrier,
                    inc=1,
                    device_id=device(p + 3, q + 3, lax.rem(me + d, 8)),
                    device_id_type=MESH_ID,
                )
                peers += 1
    for dla, dlo in ((2, 0), (0, 2)):
        pl.semaphore_signal(
            barrier, inc=1, device_id=device(dla, dlo, me), device_id_type=MESH_ID
        )
        peers += 1

    loads = []
    for i, (src, dst) in enumerate(
        (
            (enc_cell_in, enc_cell),
            (enc_node_in, enc_node),
            (dec_node_in, dec_node),
            (dec_cell_in, dec_cell),
            (enc_weight_in, enc_weight),
            (dec_weight_in, dec_weight),
            (enc_live_in, enc_live),
            (area_in, area),
            (target_t_in, target_t),
            (w_out_t_in, w_out_t),
            (node_gain_in, node_gain),
            (grid_latent_in, grid_latent),
            (mesh_latent_in, mesh_latent),
            (w_enc_in, w_enc),
            (w_up_in, w_up),
            (w_down_in, w_down),
            (w_msg_in, w_msg),
            (w_dec_in, w_dec),
        )
    ):
        loads.append(pltpu.make_async_copy(src, dst, ls.at[i]))
        loads[i].start()

    for copy in loads[:11]:
        copy.wait()

    table[...] = jnp.zeros_like(table)
    pad[...] = jnp.zeros_like(pad)

    def fill(k, carry):
        def put(block, value, slots, stride):
            pad[:, 0:slots] = value
            row = pad[0:1, :]
            for m in range(1, 8):
                row = row + pltpu.roll(pad[m : m + 1, :], m * stride, axis=1)
            table[pl.ds(block + k, 1), :] = row

        put(T_DEC_NODE, dec_node[k].astype(F32), SD, SD)
        for m in range(8):
            by_part[m, pl.ds(k, 1), :] = pad[m : m + 1, 0:128]
        put(T_DEC_CELL, dec_cell[k].astype(F32), SD, SD)
        put(T_DEC_SCALE, dec_weight[k], SD, SD)
        pad[...] = jnp.zeros_like(pad)
        put(T_ENC_CELL, enc_cell[k].astype(F32), SE, SEP)
        put(T_ENC_NODE, enc_node[k].astype(F32), SE, SEP)
        here = lax.broadcasted_iota(jnp.int32, (8, 8), 0) == lax.broadcasted_iota(
            jnp.int32, (8, 8), 1
        )
        live = jnp.sum(jnp.where(here, enc_live[k].astype(F32), 0.0), axis=1, keepdims=True)
        slot = lax.broadcasted_iota(jnp.int32, (8, SE), 1).astype(F32)
        put(T_ENC_SCALE, jnp.where(slot < live, enc_weight[k], 0.0), SE, SEP)
        return carry

    lax.fori_loop(0, 9, fill, 0)
    for b in range(4):
        table[T_AREA + b : T_AREA + b + 1, 0:128] = area[2 * b : 2 * b + 1, :]
        table[T_AREA + b : T_AREA + b + 1, 128:256] = area[2 * b + 1 : 2 * b + 2, :]
    cols[...] = table[...].T
    wo[...] = jnp.zeros_like(wo)
    wo[0:84, :] = w_out_t[...]
    target[...] = jnp.zeros_like(target)
    target[0:84, :] = target_t[...].astype(F32)
    loads[11].wait()

    def column(block, k, rows):
        turned = pltpu.roll(cols[...], lax.rem(128 - (block + k), 128), axis=1)
        return turned[0:rows, 0:1]

    def pick(block, k, rows, width):
        index = column(block, k, rows).astype(jnp.int32)
        return (index == lax.broadcasted_iota(jnp.int32, (rows, width), 1)).astype(F32).astype(BF)

    def place(block, k, rows, width):
        index = table[pl.ds(block + k, 1), :][:, 0:width].astype(jnp.int32)
        return (index == lax.broadcasted_iota(jnp.int32, (rows, width), 0)).astype(F32)

    def chunk_of(t):
        return lax.rem(4 * t + 8, 9)

    def valid(k, sign):
        at = la + sign * (k // 3 - 1)
        return (at >= 0) & (at < 4)

    def to(src, dst, slot, where):
        copy = pltpu.make_async_remote_copy(
            src_ref=src,
            dst_ref=dst,
            send_sem=gs.at[slot],
            recv_sem=gr.at[slot],
            device_id=where,
            device_id_type=MESH_ID,
        )
        copy.start()
        sent.append(copy)
        return copy

    def arrived(copies):
        for copy in copies:
            copy.wait_recv()

    sent = []
    partner = device(0, 0, me + 1 - 2 * core)

    def send(phase, k, src, dst, sign):
        dla = k // 3 - 1
        dlo = lax.rem(k, 3) - 1
        for d in (4, 3, 5, 2, 6, 1, 7, 0):
            if phase in (1, 2) and d in (3, 4, 5):
                continue
            part = lax.rem(me + d, 8)
            copy = pltpu.make_async_remote_copy(
                src_ref=src.at[k * 8 + part],
                dst_ref=dst.at[k * 8 + me],
                send_sem=ssem.at[phase, k],
                recv_sem=rsem.at[phase, k],
                device_id=device(sign * dla + 4, sign * dlo + 4, part),
                device_id_type=MESH_ID,
            )
            if d == 0:
                pl.when(k != 4)(copy.start)
            else:
                copy.start()
        if phase in (1, 2):
            part = lax.rem(me + 3 + 2 * core, 8)
            pltpu.make_async_remote_copy(
                src_ref=src.at[k * 8 + part],
                dst_ref=dst.at[k * 8 + me],
                send_sem=ssem.at[phase, k],
                recv_sem=rsem.at[phase, k],
                device_id=device(sign * dla + 4, sign * dlo + 4, part),
                device_id_type=MESH_ID,
            ).start()

    def await_bytes(sem, phase, k, buf, usual=8):
        whole = buf.at[pl.ds(k * 8, usual)]
        most = buf.at[pl.ds(k * 8, 5 if phase in (1, 2) else 7)]

        @pl.when(k != 4)
        def _():
            pltpu.make_async_copy(whole, whole, sem.at[phase, k]).wait()

        @pl.when(k == 4)
        def _():
            pltpu.make_async_copy(most, most, sem.at[phase, k]).wait()

    def own(k, src, dst):
        @pl.when(k == 4)
        def _():
            dst[4 * 8 + me] = src[4 * 8 + me]

    def put_rows(buf, k, rows_f32, slots):
        for m in range(8):
            buf[k * 8 + m] = rows_f32[m * slots : (m + 1) * slots, :].astype(BF)

    def get_rows(buf, k, slots):
        return buf[pl.ds(k * 8, 8)].astype(F32).reshape(8 * slots, W)

    def loop(body, first=0, last=9):
        def step(t, carry):
            body(chunk_of(t))
            return carry

        lax.fori_loop(first, last, step, 0)

    def enc_make(k):
        @pl.when(valid(k, 1))
        def _():
            rows = dot(pick(T_ENC_CELL, k, EROWS, CELLS), grid_latent[...])
            put_rows(es, k, rows * column(T_ENC_SCALE, k, EROWS), SEP)

    loop(enc_make, 0, 3)
    pl.semaphore_wait(barrier, peers)

    def enc_send(k):
        @pl.when(valid(k, 1))
        def _():
            send(0, k, es, ed, 1)
            own(k, es, ed)

    def enc_both(k):
        enc_make(k)
        enc_send(k)

    loop(enc_send, 0, 3)
    far_tables = [
        to(by_part.at[far_same], far_part.at[0], 27, device(0, 0, far_same)),
        to(by_part.at[far_other], far_part.at[1], 28, device(0, 0, far_other)),
    ]
    loop(enc_both, 3, 9)

    acc_n[...] = jnp.zeros_like(acc_n)

    def enc_take(k):
        @pl.when(valid(k, -1))
        def _():
            await_bytes(rsem, 0, k, ed)
            rows = get_rows(ed, k, SEP).astype(BF)
            acc_n[...] += dot(place(T_ENC_NODE, k, NODES, EROWS).astype(BF), rows)

    loop(enc_take)

    for copy in loads[12:]:
        copy.wait()
    aggb[...] = acc_n[...].astype(BF)
    state = mesh_latent[...].astype(F32) + dot(aggb[...], w_enc[...])
    nstate[...] = state
    inv_rms = lax.rsqrt(jnp.mean(state * state, axis=-1, keepdims=True) + 1e-05)
    normed[...] = (state * inv_rms * node_gain[...]).astype(BF)
    activation = dot(normed[...], w_up[...])
    act[...] = activation
    hidden[...] = (activation * sigmoid(activation)).astype(BF)
    nhalf[...] = (nstate[...] + dot(hidden[...], w_down[...])).astype(BF)
    prew[...] = dot(nhalf[...], w_msg[...]).astype(BF)

    def dec_send(k):
        @pl.when(valid(k, 1))
        def _():
            put_rows(ds_, k, dot(pick(T_DEC_NODE, k, DROWS, NODES), prew[...]), SD)
            send(1, k, ds_, dd, 1)
            own(k, ds_, dd)

    far_block = to(prew, far_rows.at[0], 29, device(0, 0, far_same))
    loop(dec_send)

    def relay(i, source):
        turned = far_part[i].T
        index = jnp.concatenate([turned[0:SD, k : k + 1] for k in range(9)], axis=0)
        width = lax.broadcasted_iota(jnp.int32, (9 * SD, NODES), 1)
        chosen = (index.astype(jnp.int32) == width).astype(F32).astype(BF)
        kept[i] = chosen
        rows = dot(chosen, far_rows[i]).astype(BF)
        for k in range(9):
            far_out[i * 9 + k] = rows[k * SD : (k + 1) * SD, :]

        def relay_send(k):
            @pl.when(valid(k, 1) & (k != 4))
            def _():
                pltpu.make_async_remote_copy(
                    src_ref=far_out.at[i * 9 + k],
                    dst_ref=dd.at[k * 8 + source],
                    send_sem=ssem.at[1, k],
                    recv_sem=rsem.at[1, k],
                    device_id=device(k // 3 + 3, lax.rem(k, 3) + 3, me),
                    device_id_type=MESH_ID,
                ).start()

        loop(relay_send)
        dd[4 * 8 + source] = far_out[i * 9 + 4]

    arrived(far_tables)
    arrived([far_block])
    far_block = to(far_rows.at[0], far_rows.at[1], 30, partner)
    relay(0, far_same)
    arrived([far_block])
    relay(1, far_other)
    acc_c[...] = jnp.zeros_like(acc_c)

    def dec_take(k):
        @pl.when(valid(k, -1))
        def _():
            await_bytes(rsem, 1, k, dd)
            pre = get_rows(dd, k, SD)
            rows = (column(T_DEC_SCALE, k, DROWS) * (pre * sigmoid(pre))).astype(BF)
            acc_c[...] += dot(place(T_DEC_CELL, k, CELLS, DROWS).astype(BF), rows)

    loop(dec_take)

    for b in range(4):
        at = pl.ds(b * 256, 256)
        gathered = acc_c[at, :].astype(BF)
        gath[at, :] = gathered
        blended = (grid_latent[at, :].astype(F32) + dot(gathered, w_dec[...])).astype(BF)
        blend[at, :] = blended
        output = dot_nt(blended, wo[...])
        weight = cols[0:256, T_AREA + b : T_AREA + b + 1]
        residual = (weight * (output - target[:, at].T)).astype(BF)
        resid[at, :] = residual
        back = dot(residual, wo[...])
        grid_grad[at, :] = back
        half = back.astype(BF)
        bhalf[at, :] = half
        bgath[at, :] = dot_nt(half, w_dec[...]).astype(BF)

    def back_send(k):
        @pl.when(valid(k, -1))
        def _():
            pre = get_rows(dd, k, SD)
            rows = dot(pick(T_DEC_CELL, k, DROWS, CELLS), bgath[...])
            put_rows(bs, k, rows * column(T_DEC_SCALE, k, DROWS) * slope(pre), SD)
            for i, source in enumerate((far_same, far_other)):
                copy = pltpu.make_async_remote_copy(
                    src_ref=bs.at[k * 8 + source],
                    dst_ref=far_in.at[i * 9 + k],
                    send_sem=ssem.at[2, k],
                    recv_sem=fsem.at[i, k],
                    device_id=device(5 - k // 3, 5 - lax.rem(k, 3), me),
                    device_id_type=MESH_ID,
                )
                pl.when(k != 4)(copy.start)

            @pl.when(k == 4)
            def _():
                far_in[4] = bs[4 * 8 + far_same]
                far_in[9 + 4] = bs[4 * 8 + far_other]

            send(2, k, bs, bd, -1)
            own(k, bs, bd)

    loop(back_send)

    def over_lat(src, dst, slot):
        return [
            to(src.at[lax.rem(la + d, 4)], dst.at[d - 1], slot + d, device(d, 0, me))
            for d in (2, 1, 3)
        ]

    def over_lon(src, dst, slot):
        return [
            to(src.at[lax.rem(lo + d, 4)], dst.at[d - 1], slot + d, device(0, d, me))
            for d in (2, 1, 3)
        ]

    scale = 1.0 / CELLS
    grad = (dot_tn(gath[...], bhalf[...]) * scale).astype(BF)
    ga[0] = grad[:, 0:384]
    ga[1, :, 0:128] = grad[:, 384:512]
    ga[1, :, 128:256] = (dot_tn(blend[...], resid[...]) * scale).astype(BF)
    ga[1, :, 256:384] = jnp.zeros((W, 128), BF)
    arrived([to(ga.at[1 - core], la_c, 0, partner)])
    for j in range(4):
        rows = pl.ds(j * 128, 128)
        ha[j] = (ga[core, rows, :].astype(F32) + la_c[rows, :].astype(F32)).astype(BF)
    wait_a = over_lat(ha, la_y, 0)

    def far_sum(i):
        def far_take(k):
            landing = far_in.at[i * 9 + k]

            @pl.when(valid(k, 1) & (k != 4))
            def _():
                pltpu.make_async_copy(landing, landing, fsem.at[i, k]).wait()

            @pl.when(jnp.logical_not(valid(k, 1)))
            def _():
                far_in[i * 9 + k] = jnp.zeros((SD, W), BF)

        loop(far_take)
        return dot_tn(kept[i], far_in[i * 9 : (i + 1) * 9].reshape(9 * SD, W))

    part_other[...] = far_sum(1).astype(BF)
    wait_part = to(part_other, part_in, 24, partner)
    total = far_sum(0)
    arrived([wait_part])
    part_out[...] = (total + part_in[...].astype(F32)).astype(BF)
    wait_far = to(part_out, far_back, 25, device(0, 0, far_same))

    acc_n[...] = jnp.zeros_like(acc_n)

    def back_take(k):
        @pl.when(valid(k, 1))
        def _():
            bd[k * 8 + far_same] = jnp.zeros((SD, W), BF)
            bd[k * 8 + far_other] = jnp.zeros((SD, W), BF)
            await_bytes(rsem, 2, k, bd, 6)
            rows = get_rows(bd, k, SD).astype(BF)
            acc_n[...] += dot(place(T_DEC_NODE, k, NODES, DROWS).astype(BF), rows)

    loop(back_take)

    arrived([wait_far])
    back_pre = (acc_n[...] + far_back[...].astype(F32)).astype(BF)
    back_node = dot_nt(back_pre, w_msg[...])
    back_node_half = back_node.astype(BF)
    back_act = (dot_nt(back_node_half, w_down[...]) * slope(act[...])).astype(BF)
    back_norm = dot_nt(back_act, w_up[...]) * node_gain[...]
    state = nstate[...]
    inv_rms = lax.rsqrt(jnp.mean(state * state, axis=-1, keepdims=True) + 1e-05)
    mean_term = jnp.mean(state * back_norm, axis=-1, keepdims=True)
    back_state = back_node + inv_rms * back_norm - state * (inv_rms * inv_rms * inv_rms * mean_term)
    back_half = back_state.astype(BF)
    backw[...] = dot_nt(back_half, w_enc[...]).astype(BF)

    def enc_back_send(k):
        @pl.when(valid(k, -1))
        def _():
            put_rows(fs, k, dot(pick(T_ENC_NODE, k, EROWS, NODES), backw[...]), SEP)
            send(3, k, fs, fd, -1)
            own(k, fs, fd)

    loop(enc_back_send, 0, 5)

    gb[0, :, 0:512] = (dot_tn(nhalf[...], back_pre) * scale).astype(BF)
    gb[0, :, 512:1024] = (dot_tn(hidden[...], back_node_half) * scale).astype(BF)
    gb[1, :, 0:512] = (dot_tn(normed[...], back_act) * scale).astype(BF)
    gb[1, :, 512:1024] = (dot_tn(aggb[...], back_half) * scale).astype(BF)
    wait_b = [to(gb.at[1 - core], lb_c, 4, partner)]
    loop(enc_back_send, 5, 9)

    arrived(wait_b)
    for j in range(4):
        rows = pl.ds(j * 128, 128)
        both = gb[core, rows, :].astype(F32) + lb_c[rows, :].astype(F32)
        hu[j] = both[:, 0:512].astype(BF)
        for i in range(4):
            hv[i, j] = both[i * 32 : (i + 1) * 32, 512:1024].astype(BF)
    wait_u = over_lat(hu, lu_y, 4)
    wait_v = over_lon(hv, lv_z, 8)
    arrived(wait_a)
    total = ha[la].astype(F32) + la_y[0].astype(F32) + la_y[1].astype(F32) + la_y[2].astype(F32)
    for j in range(4):
        ha2[j] = total[j * 32 : (j + 1) * 32, :].astype(BF)
    wait_a = over_lon(ha2, la_z, 12)

    arrived(wait_u)
    total = hu[la].astype(F32) + lu_y[0].astype(F32) + lu_y[1].astype(F32) + lu_y[2].astype(F32)
    for j in range(4):
        hu2[j] = total[j * 32 : (j + 1) * 32, :].astype(BF)
    wait_u = over_lon(hu2, lu_z, 16)
    arrived(wait_v)
    for j in range(4):
        total = hv[lo, j].astype(F32) + lv_z[0, j].astype(F32)
        hv2[j] = (total + lv_z[1, j].astype(F32) + lv_z[2, j].astype(F32)).astype(BF)
    wait_v = over_lat(hv2, lv_y, 20)

    def finished(own_part, landed):
        total = own_part.astype(F32) + landed[0].astype(F32)
        return total + landed[1].astype(F32) + landed[2].astype(F32)

    arrived(wait_u)
    arrived(wait_v)
    arrived(wait_a)
    for at, total in (
        (0, finished(hu2[lo], lu_z)),
        (512, finished(hv2[la], lv_y)),
        (1024, finished(ha2[lo], la_z)),
    ):
        for j in range(8):
            hm[j, :, at : at + total.shape[1]] = total[j * 4 : (j + 1) * 4, :].astype(BF)
    wait_m = []
    for d in (4, 3, 5, 2, 6, 1, 7):
        part = lax.rem(me + d, 8)
        wait_m.append(to(hm.at[part], lm.at[d - 1], 32 + d, device(0, 0, part)))

    def enc_back_take(k):
        @pl.when(valid(k, 1))
        def _():
            await_bytes(rsem, 3, k, fd)
            rows = get_rows(fd, k, SEP).astype(BF)
            weight = table[pl.ds(T_ENC_SCALE + k, 1), :][:, 0:EROWS]
            spread = (place(T_ENC_CELL, k, CELLS, EROWS) * weight).astype(BF)
            grid_grad[...] += dot(spread, rows)

    loop(enc_back_take, 0, 8)

    await_bytes(rsem, 3, 4, fd)
    rows = get_rows(fd, 4, SEP).astype(BF)
    weight = table[T_ENC_SCALE + 4 : T_ENC_SCALE + 5, 0:EROWS]
    index = table[T_ENC_CELL + 4 : T_ENC_CELL + 5, 0:EROWS].astype(jnp.int32)
    leave = []
    for b in range(4):
        at = pl.ds(b * 256, 256)
        here = index == lax.broadcasted_iota(jnp.int32, (256, EROWS), 0) + b * 256
        spread = (here.astype(F32) * weight).astype(BF)
        grid_half[at, :] = (grid_grad[at, :] + dot(spread, rows)).astype(BF)
        leave.append(pltpu.make_async_copy(grid_half.at[at], grid_out.at[at], os_.at[b]))
        leave[b].start()

    arrived(wait_m)
    landed = [lm[d].astype(F32) for d in range(7)]
    same = hm[me].astype(F32)
    other = landed[0]
    same = same + landed[1] + landed[3] + landed[5]
    other = other + landed[2] + landed[4] + landed[6]
    low = jnp.where(core == 0, same, other)
    high = jnp.where(core == 0, other, same)
    g_msg[...] = low[:, 0:512]
    g_down[...] = low[:, 512:1024]
    g_dec[:, 0:384] = low[:, 1024:1408]
    g_up[...] = high[:, 0:512]
    g_enc[...] = high[:, 512:1024]
    g_dec[:, 384:512] = high[:, 1024:1152]
    g_out[...] = high[:, 1152 : 1152 + 84]

    for c in sent:
        c.wait_send()
    for c in leave:
        c.wait()

    def drain(k):
        @pl.when(valid(k, 1))
        def _():
            await_bytes(ssem, 0, k, es)
            await_bytes(ssem, 1, k, ds_)

        @pl.when(valid(k, -1))
        def _():
            await_bytes(ssem, 2, k, bs)
            await_bytes(ssem, 3, k, fs)

    loop(drain)


def scratch():
    v = pltpu.VMEM
    return [
        v((9, 8, SE), jnp.int32),
        v((9, 8, SE), jnp.int32),
        v((9, 8, SD), jnp.int32),
        v((9, 8, SD), jnp.int32),
        v((9, 8, SE), F32),
        v((9, 8, SD), F32),
        v((9, 1, 8), jnp.int32),
        v((8, 128), F32),
        v((84, CELLS), BF),
        v((84, W), BF),
        v((1, W), F32),
        v((CELLS, W), BF),
        v((NODES, W), BF),
        v((W, W), BF),
        v((W, W), BF),
        v((W, W), BF),
        v((W, W), BF),
        v((W, W), BF),
        v((128, CELLS), F32),
        v((8, 256), F32),
        v((128, 256), F32),
        v((256, 128), F32),
        v((CELLS, W), F32),
        v((CELLS, W), BF),
        pltpu.SemaphoreType.DMA((4,)),
        v((8, 16, 128), F32),
        v((2, 16, 128), F32),
        v((2, NODES, W), BF),
        v((18, SD, W), BF),
        v((NODES, W), BF),
        v((2, 9 * SD, NODES), BF),
        v((18, SD, W), BF),
        v((NODES, W), BF),
        v((NODES, W), BF),
        v((NODES, W), BF),
        v((NODES, W), BF),
        pltpu.SemaphoreType.DMA((2, 9)),
        v((72, SEP, W), BF),
        v((72, SEP, W), BF),
        v((72, SD, W), BF),
        v((72, SD, W), BF),
        v((72, SD, W), BF),
        v((72, SD, W), BF),
        v((72, SEP, W), BF),
        v((72, SEP, W), BF),
        v((NODES, W), F32),
        v((CELLS, W), F32),
        v((CELLS, W), BF),
        v((CELLS, W), BF),
        v((CELLS, W), BF),
        v((CELLS, W), BF),
        v((CELLS, 128), BF),
        v((128, W), BF),
        v((NODES, W), F32),
        v((NODES, W), F32),
        v((NODES, W), BF),
        v((NODES, W), BF),
        v((NODES, W), BF),
        v((NODES, W), BF),
        v((NODES, W), BF),
        v((2, W, 384), BF),
        v((W, 384), BF),
        v((4, 128, 384), BF),
        v((3, 128, 384), BF),
        v((4, 32, 384), BF),
        v((3, 32, 384), BF),
        v((2, W, 1024), BF),
        v((W, 1024), BF),
        v((4, 128, 512), BF),
        v((3, 128, 512), BF),
        v((4, 32, 512), BF),
        v((3, 32, 512), BF),
        v((4, 4, 32, 512), BF),
        v((3, 4, 32, 512), BF),
        v((4, 32, 512), BF),
        v((3, 32, 512), BF),
        v((8, 4, 1408), BF),
        v((7, 4, 1408), BF),
        pltpu.SemaphoreType.DMA((4, 9)),
        pltpu.SemaphoreType.DMA((4, 9)),
        pltpu.SemaphoreType.DMA((40,)),
        pltpu.SemaphoreType.DMA((40,)),
        pltpu.SemaphoreType.DMA((18,)),
    ]


def on_device(
    grid_latent,
    target,
    area,
    mesh_latent,
    node_gain,
    w_enc,
    w_up,
    w_down,
    w_msg,
    w_dec,
    w_out,
    enc_cell,
    enc_live,
    enc_weight,
    enc_node,
    dec_node,
    dec_cell,
    dec_weight,
):
    vm = pl.BlockSpec(memory_space=pltpu.VMEM)
    small = jax.ShapeDtypeStruct((4, W), F32)
    any_space = pl.BlockSpec(memory_space=pl.ANY)
    rest = (small,) * 5 + (jax.ShapeDtypeStruct((4, 84), F32),)
    outs = pl.pallas_call(
        kernel,
        out_shape=(jax.ShapeDtypeStruct((CELLS, W), BF),) + rest,
        in_specs=[any_space] * 18,
        out_specs=(any_space,) + (vm,) * 6,
        scratch_shapes=scratch(),
        compiler_params=pltpu.CompilerParams(
            collective_id=0, has_side_effects=True, vmem_limit_bytes=VMEM_LIMIT
        ),
        name="step",
    )(
        enc_cell.reshape(9, 8, SE),
        enc_node.reshape(9, 8, SE),
        dec_node.reshape(9, 8, SD),
        dec_cell.reshape(9, 8, SD),
        enc_weight.reshape(9, 8, SE),
        dec_weight.reshape(9, 8, SD),
        enc_live.reshape(9, 1, 8),
        area.reshape(8, 128),
        target.T,
        w_out.T,
        node_gain.reshape(1, W),
        grid_latent,
        mesh_latent,
        w_enc,
        w_up,
        w_down,
        w_msg,
        w_dec,
    )
    return pl.pallas_call(
        finish,
        out_shape=(jax.ShapeDtypeStruct((CELLS, W), F32),) + rest,
        in_specs=[any_space] * 7,
        out_specs=(any_space,) * 7,
        scratch_shapes=[
            pltpu.VMEM((CELLS, W), BF),
            pltpu.VMEM((CELLS, W), F32),
            pltpu.VMEM((5, 4, W), F32),
            pltpu.VMEM((4, 84), F32),
            pltpu.SemaphoreType.DMA((10,)),
            pltpu.SemaphoreType.DMA((10,)),
        ],
        compiler_params=pltpu.CompilerParams(vmem_limit_bytes=VMEM_LIMIT),
        name="finish",
    )(*outs)


def finish(*refs):
    half, full, small, head, arrive, leave = refs[14:]
    blocks = [pl.ds(b * 256, 256) for b in range(4)]
    inward = [(refs[0].at[rows], half.at[rows]) for rows in blocks]
    inward += [(refs[i], small.at[i - 1]) for i in range(1, 6)] + [(refs[6], head)]
    outward = [(full.at[rows], refs[7].at[rows]) for rows in blocks]
    outward += [(small.at[i - 1], refs[7 + i]) for i in range(1, 6)] + [(head, refs[13])]
    inward = [pltpu.make_async_copy(a, b, arrive.at[i]) for i, (a, b) in enumerate(inward)]
    outward = [pltpu.make_async_copy(a, b, leave.at[i]) for i, (a, b) in enumerate(outward)]
    for copy in inward:
        copy.start()
    for i in range(10):
        inward[i].wait()
        if i < 4:
            full[blocks[i], :] = half[blocks[i], :].astype(F32)
        outward[i].start()
    for copy in outward:
        copy.wait()


def solution(mesh):
    rows = P(AXES, None)
    slots = P(AXES, None, None, None, None)
    in_specs = (
        rows,
        rows,
        P(AXES),
        rows,
        P(),
        P(),
        P(),
        P(),
        P(),
        P(),
        P(),
        slots,
        P(AXES, None, None, None),
        slots,
        slots,
        slots,
        slots,
        slots,
    )
    return jax.shard_map(
        on_device, mesh=mesh, in_specs=in_specs, out_specs=(rows,) * 7, check_vma=False
    )
```

```python
import jax
import jax.numpy as jnp
from jax import lax
from jax.experimental import pallas as pl
from jax.experimental.pallas import tpu as pltpu
from jax.sharding import PartitionSpec as P

AXES = ("lat", "lon", "mesh")
MESH_ID = pl.DeviceIdType.MESH
W = 512
CELLS = 1024
NODES = 320
SE = 21
SEP = 24
SD = 32
EROWS = 8 * SEP
DROWS = 8 * SD
T_ENC_CELL, T_ENC_NODE, T_DEC_NODE, T_DEC_CELL, T_ENC_SCALE, T_DEC_SCALE, T_AREA = (
    0,
    9,
    18,
    27,
    36,
    45,
    54,
)
VMEM_LIMIT = 67043328
BF = jnp.bfloat16
F32 = jnp.float32


def dot(a, b):
    return jnp.dot(a, b, preferred_element_type=F32)


def dot_nt(a, b):
    return lax.dot_general(a, b, (((1,), (1,)), ((), ())), preferred_element_type=F32)


def dot_tn(a, b):
    return lax.dot_general(a, b, (((0,), (0,)), ((), ())), preferred_element_type=F32)


def sigmoid(x):
    return 0.5 * jnp.tanh(0.5 * x) + 0.5


def slope(x):
    s = sigmoid(x)
    return s * (1.0 + x * (1.0 - s))


def kernel(
    enc_cell_in,
    enc_node_in,
    dec_node_in,
    dec_cell_in,
    enc_weight_in,
    dec_weight_in,
    enc_live_in,
    area_in,
    target_t_in,
    w_out_t_in,
    node_gain_in,
    grid_latent_in,
    mesh_latent_in,
    w_enc_in,
    w_up_in,
    w_down_in,
    w_msg_in,
    w_dec_in,
    grid_out,
    g_enc,
    g_up,
    g_down,
    g_msg,
    g_dec,
    g_out,
    enc_cell,
    enc_node,
    dec_node,
    dec_cell,
    enc_weight,
    dec_weight,
    enc_live,
    area,
    target_t,
    w_out_t,
    node_gain,
    grid_latent,
    mesh_latent,
    w_enc,
    w_up,
    w_down,
    w_msg,
    w_dec,
    target,
    pad,
    table,
    cols,
    grid_grad,
    grid_half,
    through,
    base,
    os_,
    by_part,
    far_part,
    far_rows,
    far_out,
    backw,
    es,
    ed,
    ds_,
    dd,
    bs,
    bd,
    fs,
    fd,
    acc_n,
    acc_c,
    gath,
    blend,
    bhalf,
    bgath,
    resid,
    wo,
    nstate,
    act,
    normed,
    hidden,
    nhalf,
    prew,
    aggb,
    ga,
    la_c,
    ha,
    la_y,
    ha2,
    la_z,
    gb,
    lb_c,
    hu,
    lu_y,
    hu2,
    lu_z,
    hv,
    lv_z,
    hv2,
    lv_y,
    hm,
    lm,
    ssem,
    rsem,
    gs,
    gr,
    ls,
):
    la, lo, me = lax.axis_index("lat"), lax.axis_index("lon"), lax.axis_index("mesh")
    core = lax.rem(me, 2)
    far_same = lax.rem(me + 4, 8)
    far_other = far_same + 1 - 2 * core

    def device(dla, dlo, part):
        return {"lat": lax.rem(la + dla, 4), "lon": lax.rem(lo + dlo, 4), "mesh": part}

    barrier = pltpu.get_barrier_semaphore()
    peers = 0
    for p in range(3):
        for q in range(3):
            for d in range(8):
                if p == 1 and q == 1 and d == 0:
                    continue
                pl.semaphore_signal(
                    barrier,
                    inc=1,
                    device_id=device(p + 3, q + 3, lax.rem(me + d, 8)),
                    device_id_type=MESH_ID,
                )
                peers += 1
    for dla, dlo in ((2, 0), (0, 2)):
        pl.semaphore_signal(
            barrier, inc=1, device_id=device(dla, dlo, me), device_id_type=MESH_ID
        )
        peers += 1

    loads = []
    for i, (src, dst) in enumerate(
        (
            (enc_cell_in, enc_cell),
            (enc_node_in, enc_node),
            (dec_node_in, dec_node),
            (dec_cell_in, dec_cell),
            (enc_weight_in, enc_weight),
            (dec_weight_in, dec_weight),
            (enc_live_in, enc_live),
            (area_in, area),
            (target_t_in, target_t),
            (w_out_t_in, w_out_t),
            (node_gain_in, node_gain),
            (grid_latent_in, grid_latent),
            (mesh_latent_in, mesh_latent),
            (w_enc_in, w_enc),
            (w_up_in, w_up),
            (w_down_in, w_down),
            (w_msg_in, w_msg),
            (w_dec_in, w_dec),
        )
    ):
        loads.append(pltpu.make_async_copy(src, dst, ls.at[i]))
        loads[i].start()

    for copy in loads[:11]:
        copy.wait()

    table[...] = jnp.zeros_like(table)
    pad[...] = jnp.zeros_like(pad)

    def fill(k, carry):
        def put(block, value, slots, stride):
            pad[:, 0:slots] = value
            row = pad[0:1, :]
            for m in range(1, 8):
                row = row + pltpu.roll(pad[m : m + 1, :], m * stride, axis=1)
            table[pl.ds(block + k, 1), :] = row

        put(T_DEC_NODE, dec_node[k].astype(F32), SD, SD)
        for m in range(8):
            by_part[m, pl.ds(k, 1), :] = pad[m : m + 1, 0:128]
        put(T_DEC_CELL, dec_cell[k].astype(F32), SD, SD)
        put(T_DEC_SCALE, dec_weight[k], SD, SD)
        pad[...] = jnp.zeros_like(pad)
        put(T_ENC_CELL, enc_cell[k].astype(F32), SE, SEP)
        put(T_ENC_NODE, enc_node[k].astype(F32), SE, SEP)
        here = lax.broadcasted_iota(jnp.int32, (8, 8), 0) == lax.broadcasted_iota(
            jnp.int32, (8, 8), 1
        )
        live = jnp.sum(jnp.where(here, enc_live[k].astype(F32), 0.0), axis=1, keepdims=True)
        slot = lax.broadcasted_iota(jnp.int32, (8, SE), 1).astype(F32)
        put(T_ENC_SCALE, jnp.where(slot < live, enc_weight[k], 0.0), SE, SEP)
        return carry

    lax.fori_loop(0, 9, fill, 0)
    for b in range(4):
        table[T_AREA + b : T_AREA + b + 1, 0:128] = area[2 * b : 2 * b + 1, :]
        table[T_AREA + b : T_AREA + b + 1, 128:256] = area[2 * b + 1 : 2 * b + 2, :]
    cols[...] = table[...].T
    wo[...] = jnp.zeros_like(wo)
    wo[0:84, :] = w_out_t[...]
    target[...] = jnp.zeros_like(target)
    target[0:84, :] = target_t[...].astype(F32)
    loads[11].wait()

    def column(block, k, rows):
        turned = pltpu.roll(cols[...], lax.rem(128 - (block + k), 128), axis=1)
        return turned[0:rows, 0:1]

    def pick(block, k, rows, width):
        index = column(block, k, rows).astype(jnp.int32)
        return (index == lax.broadcasted_iota(jnp.int32, (rows, width), 1)).astype(F32).astype(BF)

    def place(block, k, rows, width):
        index = table[pl.ds(block + k, 1), :][:, 0:width].astype(jnp.int32)
        return (index == lax.broadcasted_iota(jnp.int32, (rows, width), 0)).astype(F32)

    def chunk_of(t):
        return lax.rem(4 * t + 8, 9)

    def valid(k, sign):
        at = la + sign * (k // 3 - 1)
        return (at >= 0) & (at < 4)

    def to(src, dst, slot, where):
        copy = pltpu.make_async_remote_copy(
            src_ref=src,
            dst_ref=dst,
            send_sem=gs.at[slot],
            recv_sem=gr.at[slot],
            device_id=where,
            device_id_type=MESH_ID,
        )
        copy.start()
        sent.append(copy)
        return copy

    def arrived(copies):
        for copy in copies:
            copy.wait_recv()

    sent = []
    partner = device(0, 0, me + 1 - 2 * core)

    def send(phase, k, src, dst, sign):
        dla = k // 3 - 1
        dlo = lax.rem(k, 3) - 1
        for d in (4, 3, 5, 2, 6, 1, 7, 0):
            if phase == 1 and d in (3, 4, 5):
                continue
            part = lax.rem(me + d, 8)
            copy = pltpu.make_async_remote_copy(
                src_ref=src.at[k * 8 + part],
                dst_ref=dst.at[k * 8 + me],
                send_sem=ssem.at[phase, k],
                recv_sem=rsem.at[phase, k],
                device_id=device(sign * dla + 4, sign * dlo + 4, part),
                device_id_type=MESH_ID,
            )
            if d == 0:
                pl.when(k != 4)(copy.start)
            else:
                copy.start()
        if phase == 1:
            part = lax.rem(me + 3 + 2 * core, 8)
            pltpu.make_async_remote_copy(
                src_ref=src.at[k * 8 + part],
                dst_ref=dst.at[k * 8 + me],
                send_sem=ssem.at[phase, k],
                recv_sem=rsem.at[phase, k],
                device_id=device(sign * dla + 4, sign * dlo + 4, part),
                device_id_type=MESH_ID,
            ).start()

    def await_bytes(sem, phase, k, buf):
        whole = buf.at[pl.ds(k * 8, 8)]
        most = buf.at[pl.ds(k * 8, 5 if phase == 1 else 7)]

        @pl.when(k != 4)
        def _():
            pltpu.make_async_copy(whole, whole, sem.at[phase, k]).wait()

        @pl.when(k == 4)
        def _():
            pltpu.make_async_copy(most, most, sem.at[phase, k]).wait()

    def own(k, src, dst):
        @pl.when(k == 4)
        def _():
            dst[4 * 8 + me] = src[4 * 8 + me]

    def put_rows(buf, k, rows_f32, slots):
        for m in range(8):
            buf[k * 8 + m] = rows_f32[m * slots : (m + 1) * slots, :].astype(BF)

    def get_rows(buf, k, slots):
        return buf[pl.ds(k * 8, 8)].astype(F32).reshape(8 * slots, W)

    def loop(body, first=0, last=9):
        def step(t, carry):
            body(chunk_of(t))
            return carry

        lax.fori_loop(first, last, step, 0)

    def enc_make(k):
        @pl.when(valid(k, 1))
        def _():
            rows = dot(pick(T_ENC_CELL, k, EROWS, CELLS), grid_latent[...])
            put_rows(es, k, rows * column(T_ENC_SCALE, k, EROWS), SEP)

    loop(enc_make, 0, 3)
    pl.semaphore_wait(barrier, peers)

    def enc_send(k):
        @pl.when(valid(k, 1))
        def _():
            send(0, k, es, ed, 1)
            own(k, es, ed)

    def enc_both(k):
        enc_make(k)
        enc_send(k)

    loop(enc_send, 0, 3)
    far_tables = [
        to(by_part.at[far_same], far_part.at[0], 27, device(0, 0, far_same)),
        to(by_part.at[far_other], far_part.at[1], 28, device(0, 0, far_other)),
    ]
    loop(enc_both, 3, 9)

    acc_n[...] = jnp.zeros_like(acc_n)

    def enc_take(k):
        @pl.when(valid(k, -1))
        def _():
            spread = place(T_ENC_NODE, k, NODES, EROWS).astype(BF)
            await_bytes(rsem, 0, k, ed)
            acc_n[...] += dot(spread, get_rows(ed, k, SEP).astype(BF))

    loop(enc_take)

    for copy in loads[12:]:
        copy.wait()
    aggb[...] = acc_n[...].astype(BF)
    state = mesh_latent[...].astype(F32) + dot(aggb[...], w_enc[...])
    nstate[...] = state
    inv_rms = lax.rsqrt(jnp.mean(state * state, axis=-1, keepdims=True) + 1e-05)
    normed[...] = (state * inv_rms * node_gain[...]).astype(BF)
    activation = dot(normed[...], w_up[...])
    act[...] = activation
    hidden[...] = (activation * sigmoid(activation)).astype(BF)
    nhalf[...] = (nstate[...] + dot(hidden[...], w_down[...])).astype(BF)
    prew[...] = dot(nhalf[...], w_msg[...]).astype(BF)

    def dec_send(k):
        @pl.when(valid(k, 1))
        def _():
            put_rows(ds_, k, dot(pick(T_DEC_NODE, k, DROWS, NODES), prew[...]), SD)
            send(1, k, ds_, dd, 1)
            own(k, ds_, dd)

    far_block = to(prew, far_rows.at[0], 29, device(0, 0, far_same))
    loop(dec_send)

    def relay(i, source):
        turned = far_part[i].T
        index = jnp.concatenate([turned[0:SD, k : k + 1] for k in range(9)], axis=0)
        width = lax.broadcasted_iota(jnp.int32, (9 * SD, NODES), 1)
        chosen = (index.astype(jnp.int32) == width).astype(F32).astype(BF)
        rows = dot(chosen, far_rows[i]).astype(BF)
        for k in range(9):
            far_out[i * 9 + k] = rows[k * SD : (k + 1) * SD, :]

        def relay_send(k):
            @pl.when(valid(k, 1) & (k != 4))
            def _():
                pltpu.make_async_remote_copy(
                    src_ref=far_out.at[i * 9 + k],
                    dst_ref=dd.at[k * 8 + source],
                    send_sem=ssem.at[1, k],
                    recv_sem=rsem.at[1, k],
                    device_id=device(k // 3 + 3, lax.rem(k, 3) + 3, me),
                    device_id_type=MESH_ID,
                ).start()

        loop(relay_send)
        dd[4 * 8 + source] = far_out[i * 9 + 4]

    through[...] = dot_nt(wo[...], w_dec[...]).astype(BF)
    base[...] = dot_nt(grid_latent[...], wo[...]) - target[...].T

    arrived(far_tables)
    arrived([far_block])
    far_block = to(far_rows.at[0], far_rows.at[1], 30, partner)
    relay(0, far_same)
    arrived([far_block])
    relay(1, far_other)
    acc_c[...] = jnp.zeros_like(acc_c)

    def dec_take(k):
        @pl.when(valid(k, -1))
        def _():
            spread = place(T_DEC_CELL, k, CELLS, DROWS).astype(BF)
            weight = column(T_DEC_SCALE, k, DROWS)
            await_bytes(rsem, 1, k, dd)
            pre = get_rows(dd, k, SD)
            acc_c[...] += dot(spread, (weight * (pre * sigmoid(pre))).astype(BF))

    loop(dec_take)

    for b in range(4):
        at = pl.ds(b * 256, 256)
        gathered = acc_c[at, :].astype(BF)
        gath[at, :] = gathered
        weight = cols[0:256, T_AREA + b : T_AREA + b + 1]
        residual = (weight * (base[at, :] + dot_nt(gathered, through[...]))).astype(BF)
        resid[at, :] = residual
        bgath[at, :] = dot(residual, through[...]).astype(BF)

    def back_send(k):
        @pl.when(valid(k, -1))
        def _():
            pre = get_rows(dd, k, SD)
            rows = dot(pick(T_DEC_CELL, k, DROWS, CELLS), bgath[...])
            put_rows(bs, k, rows * column(T_DEC_SCALE, k, DROWS) * slope(pre), SD)
            send(2, k, bs, bd, -1)
            own(k, bs, bd)

    loop(back_send)

    for b in range(4):
        at = pl.ds(b * 256, 256)
        blend[at, :] = (grid_latent[at, :].astype(F32) + dot(gath[at, :], w_dec[...])).astype(BF)
        back = dot(resid[at, :], wo[...])
        grid_grad[at, :] = back
        bhalf[at, :] = back.astype(BF)

    def over_lat(src, dst, slot):
        return [
            to(src.at[lax.rem(la + d, 4)], dst.at[d - 1], slot + d, device(d, 0, me))
            for d in (2, 1, 3)
        ]

    def over_lon(src, dst, slot):
        return [
            to(src.at[lax.rem(lo + d, 4)], dst.at[d - 1], slot + d, device(0, d, me))
            for d in (2, 1, 3)
        ]

    scale = 1.0 / CELLS
    grad = (dot_tn(gath[...], bhalf[...]) * scale).astype(BF)
    ga[0] = grad[:, 0:384]
    ga[1, :, 0:128] = grad[:, 384:512]
    ga[1, :, 128:256] = (dot_tn(blend[...], resid[...]) * scale).astype(BF)
    ga[1, :, 256:384] = jnp.zeros((W, 128), BF)
    arrived([to(ga.at[1 - core], la_c, 0, partner)])
    for j in range(4):
        rows = pl.ds(j * 128, 128)
        ha[j] = (ga[core, rows, :].astype(F32) + la_c[rows, :].astype(F32)).astype(BF)
    wait_a = over_lat(ha, la_y, 0)

    acc_n[...] = jnp.zeros_like(acc_n)

    def back_take(k):
        @pl.when(valid(k, 1))
        def _():
            spread = place(T_DEC_NODE, k, NODES, DROWS).astype(BF)
            await_bytes(rsem, 2, k, bd)
            acc_n[...] += dot(spread, get_rows(bd, k, SD).astype(BF))

    loop(back_take)

    back_pre = acc_n[...].astype(BF)
    back_node = dot_nt(back_pre, w_msg[...])
    back_node_half = back_node.astype(BF)
    back_act = (dot_nt(back_node_half, w_down[...]) * slope(act[...])).astype(BF)
    back_norm = dot_nt(back_act, w_up[...]) * node_gain[...]
    state = nstate[...]
    inv_rms = lax.rsqrt(jnp.mean(state * state, axis=-1, keepdims=True) + 1e-05)
    mean_term = jnp.mean(state * back_norm, axis=-1, keepdims=True)
    back_state = back_node + inv_rms * back_norm - state * (inv_rms * inv_rms * inv_rms * mean_term)
    back_half = back_state.astype(BF)
    backw[...] = dot_nt(back_half, w_enc[...]).astype(BF)

    def enc_back_send(k):
        @pl.when(valid(k, -1))
        def _():
            put_rows(fs, k, dot(pick(T_ENC_NODE, k, EROWS, NODES), backw[...]), SEP)
            send(3, k, fs, fd, -1)
            own(k, fs, fd)

    loop(enc_back_send, 0, 5)

    gb[0, :, 0:512] = (dot_tn(nhalf[...], back_pre) * scale).astype(BF)
    gb[0, :, 512:1024] = (dot_tn(hidden[...], back_node_half) * scale).astype(BF)
    gb[1, :, 0:512] = (dot_tn(normed[...], back_act) * scale).astype(BF)
    gb[1, :, 512:1024] = (dot_tn(aggb[...], back_half) * scale).astype(BF)
    wait_b = [to(gb.at[1 - core], lb_c, 4, partner)]
    loop(enc_back_send, 5, 9)

    arrived(wait_b)
    for j in range(4):
        rows = pl.ds(j * 128, 128)
        both = gb[core, rows, :].astype(F32) + lb_c[rows, :].astype(F32)
        hu[j] = both[:, 0:512].astype(BF)
        for i in range(4):
            hv[i, j] = both[i * 32 : (i + 1) * 32, 512:1024].astype(BF)
    wait_u = over_lat(hu, lu_y, 4)
    wait_v = over_lon(hv, lv_z, 8)
    arrived(wait_a)
    total = ha[la].astype(F32) + la_y[0].astype(F32) + la_y[1].astype(F32) + la_y[2].astype(F32)
    for j in range(4):
        ha2[j] = total[j * 32 : (j + 1) * 32, :].astype(BF)
    wait_a = over_lon(ha2, la_z, 12)

    arrived(wait_u)
    total = hu[la].astype(F32) + lu_y[0].astype(F32) + lu_y[1].astype(F32) + lu_y[2].astype(F32)
    for j in range(4):
        hu2[j] = total[j * 32 : (j + 1) * 32, :].astype(BF)
    wait_u = over_lon(hu2, lu_z, 16)
    arrived(wait_v)
    for j in range(4):
        total = hv[lo, j].astype(F32) + lv_z[0, j].astype(F32)
        hv2[j] = (total + lv_z[1, j].astype(F32) + lv_z[2, j].astype(F32)).astype(BF)
    wait_v = over_lat(hv2, lv_y, 20)

    def finished(own_part, landed):
        total = own_part.astype(F32) + landed[0].astype(F32)
        return total + landed[1].astype(F32) + landed[2].astype(F32)

    arrived(wait_u)
    arrived(wait_v)
    arrived(wait_a)
    for at, total in (
        (0, finished(hu2[lo], lu_z)),
        (512, finished(hv2[la], lv_y)),
        (1024, finished(ha2[lo], la_z)),
    ):
        for j in range(8):
            hm[j, :, at : at + total.shape[1]] = total[j * 4 : (j + 1) * 4, :].astype(BF)
    wait_m = []
    for d in (4, 3, 5, 2, 6, 1, 7):
        part = lax.rem(me + d, 8)
        wait_m.append(to(hm.at[part], lm.at[d - 1], 32 + d, device(0, 0, part)))

    def enc_back_take(k):
        @pl.when(valid(k, 1))
        def _():
            weight = table[pl.ds(T_ENC_SCALE + k, 1), :][:, 0:EROWS]
            spread = (place(T_ENC_CELL, k, CELLS, EROWS) * weight).astype(BF)
            await_bytes(rsem, 3, k, fd)
            grid_grad[...] += dot(spread, get_rows(fd, k, SEP).astype(BF))

    loop(enc_back_take, 0, 8)

    await_bytes(rsem, 3, 4, fd)
    rows = get_rows(fd, 4, SEP).astype(BF)
    weight = table[T_ENC_SCALE + 4 : T_ENC_SCALE + 5, 0:EROWS]
    index = table[T_ENC_CELL + 4 : T_ENC_CELL + 5, 0:EROWS].astype(jnp.int32)
    leave = []
    for b in range(4):
        at = pl.ds(b * 256, 256)
        here = index == lax.broadcasted_iota(jnp.int32, (256, EROWS), 0) + b * 256
        spread = (here.astype(F32) * weight).astype(BF)
        grid_half[at, :] = (grid_grad[at, :] + dot(spread, rows)).astype(BF)
        leave.append(pltpu.make_async_copy(grid_half.at[at], grid_out.at[at], os_.at[b]))
        leave[b].start()

    arrived(wait_m)
    landed = [lm[d].astype(F32) for d in range(7)]
    same = hm[me].astype(F32)
    other = landed[0]
    same = same + landed[1] + landed[3] + landed[5]
    other = other + landed[2] + landed[4] + landed[6]
    low = jnp.where(core == 0, same, other)
    high = jnp.where(core == 0, other, same)
    g_msg[...] = low[:, 0:512]
    g_down[...] = low[:, 512:1024]
    g_dec[:, 0:384] = low[:, 1024:1408]
    g_up[...] = high[:, 0:512]
    g_enc[...] = high[:, 512:1024]
    g_dec[:, 384:512] = high[:, 1024:1152]
    g_out[...] = high[:, 1152 : 1152 + 84]

    for c in sent:
        c.wait_send()
    for c in leave:
        c.wait()

    def drain(k):
        @pl.when(valid(k, 1))
        def _():
            await_bytes(ssem, 0, k, es)
            await_bytes(ssem, 1, k, ds_)

        @pl.when(valid(k, -1))
        def _():
            await_bytes(ssem, 2, k, bs)
            await_bytes(ssem, 3, k, fs)

    loop(drain)


def scratch():
    v = pltpu.VMEM
    return [
        v((9, 8, SE), jnp.int32),
        v((9, 8, SE), jnp.int32),
        v((9, 8, SD), jnp.int32),
        v((9, 8, SD), jnp.int32),
        v((9, 8, SE), F32),
        v((9, 8, SD), F32),
        v((9, 1, 8), jnp.int32),
        v((8, 128), F32),
        v((84, CELLS), BF),
        v((84, W), BF),
        v((1, W), F32),
        v((CELLS, W), BF),
        v((NODES, W), BF),
        v((W, W), BF),
        v((W, W), BF),
        v((W, W), BF),
        v((W, W), BF),
        v((W, W), BF),
        v((128, CELLS), F32),
        v((8, 256), F32),
        v((128, 256), F32),
        v((256, 128), F32),
        v((CELLS, W), F32),
        v((CELLS, W), BF),
        v((128, W), BF),
        v((CELLS, 128), F32),
        pltpu.SemaphoreType.DMA((4,)),
        v((8, 16, 128), F32),
        v((2, 16, 128), F32),
        v((2, NODES, W), BF),
        v((18, SD, W), BF),
        v((NODES, W), BF),
        v((72, SEP, W), BF),
        v((72, SEP, W), BF),
        v((72, SD, W), BF),
        v((72, SD, W), BF),
        v((72, SD, W), BF),
        v((72, SD, W), BF),
        v((72, SEP, W), BF),
        v((72, SEP, W), BF),
        v((NODES, W), F32),
        v((CELLS, W), F32),
        v((CELLS, W), BF),
        v((CELLS, W), BF),
        v((CELLS, W), BF),
        v((CELLS, W), BF),
        v((CELLS, 128), BF),
        v((128, W), BF),
        v((NODES, W), F32),
        v((NODES, W), F32),
        v((NODES, W), BF),
        v((NODES, W), BF),
        v((NODES, W), BF),
        v((NODES, W), BF),
        v((NODES, W), BF),
        v((2, W, 384), BF),
        v((W, 384), BF),
        v((4, 128, 384), BF),
        v((3, 128, 384), BF),
        v((4, 32, 384), BF),
        v((3, 32, 384), BF),
        v((2, W, 1024), BF),
        v((W, 1024), BF),
        v((4, 128, 512), BF),
        v((3, 128, 512), BF),
        v((4, 32, 512), BF),
        v((3, 32, 512), BF),
        v((4, 4, 32, 512), BF),
        v((3, 4, 32, 512), BF),
        v((4, 32, 512), BF),
        v((3, 32, 512), BF),
        v((8, 4, 1408), BF),
        v((7, 4, 1408), BF),
        pltpu.SemaphoreType.DMA((4, 9)),
        pltpu.SemaphoreType.DMA((4, 9)),
        pltpu.SemaphoreType.DMA((40,)),
        pltpu.SemaphoreType.DMA((40,)),
        pltpu.SemaphoreType.DMA((18,)),
    ]


def on_device(
    grid_latent,
    target,
    area,
    mesh_latent,
    node_gain,
    w_enc,
    w_up,
    w_down,
    w_msg,
    w_dec,
    w_out,
    enc_cell,
    enc_live,
    enc_weight,
    enc_node,
    dec_node,
    dec_cell,
    dec_weight,
):
    vm = pl.BlockSpec(memory_space=pltpu.VMEM)
    small = jax.ShapeDtypeStruct((4, W), F32)
    any_space = pl.BlockSpec(memory_space=pl.ANY)
    rest = (small,) * 5 + (jax.ShapeDtypeStruct((4, 84), F32),)
    outs = pl.pallas_call(
        kernel,
        out_shape=(jax.ShapeDtypeStruct((CELLS, W), BF),) + rest,
        in_specs=[any_space] * 18,
        out_specs=(any_space,) + (vm,) * 6,
        scratch_shapes=scratch(),
        compiler_params=pltpu.CompilerParams(
            collective_id=0, has_side_effects=True, vmem_limit_bytes=VMEM_LIMIT
        ),
        name="step",
    )(
        enc_cell.reshape(9, 8, SE),
        enc_node.reshape(9, 8, SE),
        dec_node.reshape(9, 8, SD),
        dec_cell.reshape(9, 8, SD),
        enc_weight.reshape(9, 8, SE),
        dec_weight.reshape(9, 8, SD),
        enc_live.reshape(9, 1, 8),
        area.reshape(8, 128),
        target.T,
        w_out.T,
        node_gain.reshape(1, W),
        grid_latent,
        mesh_latent,
        w_enc,
        w_up,
        w_down,
        w_msg,
        w_dec,
    )
    return pl.pallas_call(
        finish,
        out_shape=(jax.ShapeDtypeStruct((CELLS, W), F32),) + rest,
        in_specs=[any_space] * 7,
        out_specs=(any_space,) * 7,
        scratch_shapes=[
            pltpu.VMEM((CELLS, W), BF),
            pltpu.VMEM((CELLS, W), F32),
            pltpu.VMEM((5, 4, W), F32),
            pltpu.VMEM((4, 84), F32),
            pltpu.SemaphoreType.DMA((10,)),
            pltpu.SemaphoreType.DMA((10,)),
        ],
        compiler_params=pltpu.CompilerParams(vmem_limit_bytes=VMEM_LIMIT),
        name="finish",
    )(*outs)


def finish(*refs):
    half, full, small, head, arrive, leave = refs[14:]
    blocks = [pl.ds(b * 256, 256) for b in range(4)]
    inward = [(refs[0].at[rows], half.at[rows]) for rows in blocks]
    inward += [(refs[i], small.at[i - 1]) for i in range(1, 6)] + [(refs[6], head)]
    outward = [(full.at[rows], refs[7].at[rows]) for rows in blocks]
    outward += [(small.at[i - 1], refs[7 + i]) for i in range(1, 6)] + [(head, refs[13])]
    inward = [pltpu.make_async_copy(a, b, arrive.at[i]) for i, (a, b) in enumerate(inward)]
    outward = [pltpu.make_async_copy(a, b, leave.at[i]) for i, (a, b) in enumerate(outward)]
    for copy in inward:
        copy.start()
    for i in range(10):
        inward[i].wait()
        if i < 4:
            full[blocks[i], :] = half[blocks[i], :].astype(F32)
        outward[i].start()
    for copy in outward:
        copy.wait()


def solution(mesh):
    rows = P(AXES, None)
    slots = P(AXES, None, None, None, None)
    in_specs = (
        rows,
        rows,
        P(AXES),
        rows,
        P(),
        P(),
        P(),
        P(),
        P(),
        P(),
        P(),
        slots,
        P(AXES, None, None, None),
        slots,
        slots,
        slots,
        slots,
        slots,
    )
    return jax.shard_map(
        on_device, mesh=mesh, in_specs=in_specs, out_specs=(rows,) * 7, check_vma=False
    )
```

```python
import jax
import jax.numpy as jnp
from jax import lax
from jax.experimental import pallas as pl
from jax.experimental.pallas import tpu as pltpu
from jax.sharding import PartitionSpec as P

AXES = ("lat", "lon", "mesh")
MESH_ID = pl.DeviceIdType.MESH
W = 512
CELLS = 1024
NODES = 320
SE = 21
SEP = 24
SD = 32
EROWS = 8 * SEP
DROWS = 8 * SD
T_ENC_CELL, T_ENC_NODE, T_DEC_NODE, T_DEC_CELL, T_ENC_SCALE, T_DEC_SCALE, T_AREA = (
    0,
    9,
    18,
    27,
    36,
    45,
    54,
)
VMEM_LIMIT = 67043328
BF = jnp.bfloat16
F32 = jnp.float32


def dot(a, b):
    return jnp.dot(a, b, preferred_element_type=F32)


def dot_nt(a, b):
    return lax.dot_general(a, b, (((1,), (1,)), ((), ())), preferred_element_type=F32)


def dot_tn(a, b):
    return lax.dot_general(a, b, (((0,), (0,)), ((), ())), preferred_element_type=F32)


def sigmoid(x):
    return 0.5 * jnp.tanh(0.5 * x) + 0.5


def slope(x):
    s = sigmoid(x)
    return s * (1.0 + x * (1.0 - s))


def kernel(
    enc_cell_in,
    enc_node_in,
    dec_node_in,
    dec_cell_in,
    enc_weight_in,
    dec_weight_in,
    enc_live_in,
    area_in,
    target_t_in,
    w_out_t_in,
    node_gain_in,
    grid_latent_in,
    mesh_latent_in,
    w_enc_in,
    w_up_in,
    w_down_in,
    w_msg_in,
    w_dec_in,
    grid_out,
    g_enc,
    g_up,
    g_down,
    g_msg,
    g_dec,
    g_out,
    enc_cell,
    enc_node,
    dec_node,
    dec_cell,
    enc_weight,
    dec_weight,
    enc_live,
    area,
    target_t,
    w_out_t,
    node_gain,
    grid_latent,
    mesh_latent,
    w_enc,
    w_up,
    w_down,
    w_msg,
    w_dec,
    target,
    pad,
    table,
    cols,
    grid_grad,
    grid_half,
    through,
    base,
    os_,
    by_part,
    far_part,
    far_rows,
    far_out,
    backw,
    es,
    ed,
    ds_,
    dd,
    bs,
    bd,
    fs,
    fd,
    acc_n,
    acc_c,
    gath,
    blend,
    bhalf,
    bgath,
    resid,
    wo,
    nstate,
    act,
    normed,
    hidden,
    nhalf,
    prew,
    aggb,
    ga,
    la_c,
    ha,
    la_y,
    ha2,
    la_z,
    gb,
    lb_c,
    hu,
    lu_y,
    hu2,
    lu_z,
    hv,
    lv_z,
    hv2,
    lv_y,
    hm,
    lm,
    ssem,
    rsem,
    gs,
    gr,
    ls,
):
    la, lo, me = lax.axis_index("lat"), lax.axis_index("lon"), lax.axis_index("mesh")
    core = lax.rem(me, 2)
    far_same = lax.rem(me + 4, 8)
    far_other = far_same + 1 - 2 * core

    def device(dla, dlo, part):
        return {"lat": lax.rem(la + dla, 4), "lon": lax.rem(lo + dlo, 4), "mesh": part}

    barrier = pltpu.get_barrier_semaphore()
    peers = 0
    for p in range(3):
        for q in range(3):
            for d in range(8):
                if p == 1 and q == 1 and d == 0:
                    continue
                pl.semaphore_signal(
                    barrier,
                    inc=1,
                    device_id=device(p + 3, q + 3, lax.rem(me + d, 8)),
                    device_id_type=MESH_ID,
                )
                peers += 1
    for dla, dlo in ((2, 0), (0, 2)):
        pl.semaphore_signal(
            barrier, inc=1, device_id=device(dla, dlo, me), device_id_type=MESH_ID
        )
        peers += 1

    loads = []
    for i, (src, dst) in enumerate(
        (
            (enc_cell_in, enc_cell),
            (enc_node_in, enc_node),
            (dec_node_in, dec_node),
            (dec_cell_in, dec_cell),
            (enc_weight_in, enc_weight),
            (dec_weight_in, dec_weight),
            (enc_live_in, enc_live),
            (area_in, area),
            (target_t_in, target_t),
            (w_out_t_in, w_out_t),
            (node_gain_in, node_gain),
            (grid_latent_in, grid_latent),
            (mesh_latent_in, mesh_latent),
            (w_enc_in, w_enc),
            (w_up_in, w_up),
            (w_down_in, w_down),
            (w_msg_in, w_msg),
            (w_dec_in, w_dec),
        )
    ):
        loads.append(pltpu.make_async_copy(src, dst, ls.at[i]))
        loads[i].start()

    for copy in loads[:11]:
        copy.wait()

    table[...] = jnp.zeros_like(table)
    pad[...] = jnp.zeros_like(pad)

    def fill(k, carry):
        def put(block, value, slots, stride):
            pad[:, 0:slots] = value
            row = pad[0:1, :]
            for m in range(1, 8):
                row = row + pltpu.roll(pad[m : m + 1, :], m * stride, axis=1)
            table[pl.ds(block + k, 1), :] = row

        put(T_DEC_NODE, dec_node[k].astype(F32), SD, SD)
        for m in range(8):
            by_part[m, pl.ds(k, 1), :] = pad[m : m + 1, 0:128]
        put(T_DEC_CELL, dec_cell[k].astype(F32), SD, SD)
        put(T_DEC_SCALE, dec_weight[k], SD, SD)
        pad[...] = jnp.zeros_like(pad)
        put(T_ENC_CELL, enc_cell[k].astype(F32), SE, SEP)
        put(T_ENC_NODE, enc_node[k].astype(F32), SE, SEP)
        here = lax.broadcasted_iota(jnp.int32, (8, 8), 0) == lax.broadcasted_iota(
            jnp.int32, (8, 8), 1
        )
        live = jnp.sum(jnp.where(here, enc_live[k].astype(F32), 0.0), axis=1, keepdims=True)
        slot = lax.broadcasted_iota(jnp.int32, (8, SE), 1).astype(F32)
        put(T_ENC_SCALE, jnp.where(slot < live, enc_weight[k], 0.0), SE, SEP)
        return carry

    lax.fori_loop(0, 9, fill, 0)
    for b in range(4):
        table[T_AREA + b : T_AREA + b + 1, 0:128] = area[2 * b : 2 * b + 1, :]
        table[T_AREA + b : T_AREA + b + 1, 128:256] = area[2 * b + 1 : 2 * b + 2, :]
    cols[...] = table[...].T
    wo[...] = jnp.zeros_like(wo)
    wo[0:84, :] = w_out_t[...]
    target[...] = jnp.zeros_like(target)
    target[0:84, :] = target_t[...].astype(F32)
    loads[11].wait()

    def column(block, k, rows):
        turned = pltpu.roll(cols[...], lax.rem(128 - (block + k), 128), axis=1)
        return turned[0:rows, 0:1]

    def pick(block, k, rows, width):
        index = column(block, k, rows).astype(jnp.int32)
        return (index == lax.broadcasted_iota(jnp.int32, (rows, width), 1)).astype(F32).astype(BF)

    def place(block, k, rows, width):
        index = table[pl.ds(block + k, 1), :][:, 0:width].astype(jnp.int32)
        return (index == lax.broadcasted_iota(jnp.int32, (rows, width), 0)).astype(F32)

    def chunk_of(t):
        return lax.rem(4 * t + 8, 9)

    def valid(k, sign):
        at = la + sign * (k // 3 - 1)
        return (at >= 0) & (at < 4)

    def to(src, dst, slot, where):
        copy = pltpu.make_async_remote_copy(
            src_ref=src,
            dst_ref=dst,
            send_sem=gs.at[slot],
            recv_sem=gr.at[slot],
            device_id=where,
            device_id_type=MESH_ID,
        )
        copy.start()
        sent.append(copy)
        return copy

    def arrived(copies):
        for copy in copies:
            copy.wait_recv()

    sent = []
    partner = device(0, 0, me + 1 - 2 * core)

    def send(phase, k, src, dst, sign):
        dla = k // 3 - 1
        dlo = lax.rem(k, 3) - 1
        for d in (4, 3, 5, 2, 6, 1, 7, 0):
            if phase == 1 and d in (3, 4, 5):
                continue
            part = lax.rem(me + d, 8)
            copy = pltpu.make_async_remote_copy(
                src_ref=src.at[k * 8 + part],
                dst_ref=dst.at[k * 8 + me],
                send_sem=ssem.at[phase, k],
                recv_sem=rsem.at[phase, k],
                device_id=device(sign * dla + 4, sign * dlo + 4, part),
                device_id_type=MESH_ID,
            )
            if d == 0:
                pl.when(k != 4)(copy.start)
            else:
                copy.start()
        if phase == 1:
            part = lax.rem(me + 3 + 2 * core, 8)
            pltpu.make_async_remote_copy(
                src_ref=src.at[k * 8 + part],
                dst_ref=dst.at[k * 8 + me],
                send_sem=ssem.at[phase, k],
                recv_sem=rsem.at[phase, k],
                device_id=device(sign * dla + 4, sign * dlo + 4, part),
                device_id_type=MESH_ID,
            ).start()

    def await_bytes(sem, phase, k, buf):
        whole = buf.at[pl.ds(k * 8, 8)]
        most = buf.at[pl.ds(k * 8, 5 if phase == 1 else 7)]

        @pl.when(k != 4)
        def _():
            pltpu.make_async_copy(whole, whole, sem.at[phase, k]).wait()

        @pl.when(k == 4)
        def _():
            pltpu.make_async_copy(most, most, sem.at[phase, k]).wait()

    def own(k, src, dst):
        @pl.when(k == 4)
        def _():
            dst[4 * 8 + me] = src[4 * 8 + me]

    def put_rows(buf, k, rows_f32, slots):
        for m in range(8):
            buf[k * 8 + m] = rows_f32[m * slots : (m + 1) * slots, :].astype(BF)

    def get_rows(buf, k, slots):
        return buf[pl.ds(k * 8, 8)].astype(F32).reshape(8 * slots, W)

    def loop(body, first=0, last=9):
        def step(t, carry):
            body(chunk_of(t))
            return carry

        lax.fori_loop(first, last, step, 0)

    def enc_make(k):
        @pl.when(valid(k, 1))
        def _():
            rows = dot(pick(T_ENC_CELL, k, EROWS, CELLS), grid_latent[...])
            put_rows(es, k, rows * column(T_ENC_SCALE, k, EROWS), SEP)

    loop(enc_make, 0, 3)
    pl.semaphore_wait(barrier, peers)

    def enc_send(k):
        @pl.when(valid(k, 1))
        def _():
            send(0, k, es, ed, 1)
            own(k, es, ed)

    def enc_both(k):
        enc_make(k)
        enc_send(k)

    loop(enc_send, 0, 3)
    far_tables = [
        to(by_part.at[far_same], far_part.at[0], 27, device(0, 0, far_same)),
        to(by_part.at[far_other], far_part.at[1], 28, device(0, 0, far_other)),
    ]
    loop(enc_both, 3, 9)

    acc_n[...] = jnp.zeros_like(acc_n)

    def enc_take(k):
        @pl.when(valid(k, -1))
        def _():
            spread = place(T_ENC_NODE, k, NODES, EROWS).astype(BF)
            await_bytes(rsem, 0, k, ed)
            acc_n[...] += dot(spread, get_rows(ed, k, SEP).astype(BF))

    loop(enc_take)

    for copy in loads[12:]:
        copy.wait()
    aggb[...] = acc_n[...].astype(BF)
    state = mesh_latent[...].astype(F32) + dot(aggb[...], w_enc[...])
    nstate[...] = state
    inv_rms = lax.rsqrt(jnp.mean(state * state, axis=-1, keepdims=True) + 1e-05)
    normed[...] = (state * inv_rms * node_gain[...]).astype(BF)
    activation = dot(normed[...], w_up[...])
    act[...] = activation
    hidden[...] = (activation * sigmoid(activation)).astype(BF)
    nhalf[...] = (nstate[...] + dot(hidden[...], w_down[...])).astype(BF)
    prew[...] = dot(nhalf[...], w_msg[...]).astype(BF)

    def dec_send(k):
        @pl.when(valid(k, 1))
        def _():
            put_rows(ds_, k, dot(pick(T_DEC_NODE, k, DROWS, NODES), prew[...]), SD)
            send(1, k, ds_, dd, 1)
            own(k, ds_, dd)

    far_block = to(prew, far_rows.at[0], 29, device(0, 0, far_same))
    loop(dec_send)

    def relay(i, source):
        turned = far_part[i].T
        index = jnp.concatenate([turned[0:SD, k : k + 1] for k in range(9)], axis=0)
        width = lax.broadcasted_iota(jnp.int32, (9 * SD, NODES), 1)
        chosen = (index.astype(jnp.int32) == width).astype(F32).astype(BF)
        rows = dot(chosen, far_rows[i]).astype(BF)
        for k in range(9):
            far_out[i * 9 + k] = rows[k * SD : (k + 1) * SD, :]

        def relay_send(k):
            @pl.when(valid(k, 1) & (k != 4))
            def _():
                pltpu.make_async_remote_copy(
                    src_ref=far_out.at[i * 9 + k],
                    dst_ref=dd.at[k * 8 + source],
                    send_sem=ssem.at[1, k],
                    recv_sem=rsem.at[1, k],
                    device_id=device(k // 3 + 3, lax.rem(k, 3) + 3, me),
                    device_id_type=MESH_ID,
                ).start()

        loop(relay_send)
        dd[4 * 8 + source] = far_out[i * 9 + 4]

    through[...] = dot_nt(wo[...], w_dec[...]).astype(BF)
    base[...] = dot_nt(grid_latent[...], wo[...]) - target[...].T

    arrived(far_tables)
    arrived([far_block])
    far_block = to(far_rows.at[0], far_rows.at[1], 30, partner)
    relay(0, far_same)
    arrived([far_block])
    relay(1, far_other)
    acc_c[...] = jnp.zeros_like(acc_c)

    def dec_take(k):
        @pl.when(valid(k, -1))
        def _():
            weight = column(T_DEC_SCALE, k, DROWS)
            await_bytes(rsem, 1, k, dd)
            pre = get_rows(dd, k, SD)
            rows = (weight * (pre * sigmoid(pre))).astype(BF)
            acc_c[...] += dot(place(T_DEC_CELL, k, CELLS, DROWS).astype(BF), rows)

    loop(dec_take)

    for b in range(4):
        at = pl.ds(b * 256, 256)
        gathered = acc_c[at, :].astype(BF)
        gath[at, :] = gathered
        weight = cols[0:256, T_AREA + b : T_AREA + b + 1]
        residual = (weight * (base[at, :] + dot_nt(gathered, through[...]))).astype(BF)
        resid[at, :] = residual
        bgath[at, :] = dot(residual, through[...]).astype(BF)

    def back_send(k):
        @pl.when(valid(k, -1))
        def _():
            pre = get_rows(dd, k, SD)
            rows = dot(pick(T_DEC_CELL, k, DROWS, CELLS), bgath[...])
            put_rows(bs, k, rows * column(T_DEC_SCALE, k, DROWS) * slope(pre), SD)
            send(2, k, bs, bd, -1)
            own(k, bs, bd)

    loop(back_send)

    for b in range(4):
        at = pl.ds(b * 256, 256)
        blend[at, :] = (grid_latent[at, :].astype(F32) + dot(gath[at, :], w_dec[...])).astype(BF)
        back = dot(resid[at, :], wo[...])
        grid_grad[at, :] = back
        bhalf[at, :] = back.astype(BF)

    def over_lat(src, dst, slot):
        return [
            to(src.at[lax.rem(la + d, 4)], dst.at[d - 1], slot + d, device(d, 0, me))
            for d in (2, 1, 3)
        ]

    def over_lon(src, dst, slot):
        return [
            to(src.at[lax.rem(lo + d, 4)], dst.at[d - 1], slot + d, device(0, d, me))
            for d in (2, 1, 3)
        ]

    scale = 1.0 / CELLS
    grad = (dot_tn(gath[...], bhalf[...]) * scale).astype(BF)
    ga[0] = grad[:, 0:384]
    ga[1, :, 0:128] = grad[:, 384:512]
    ga[1, :, 128:256] = (dot_tn(blend[...], resid[...]) * scale).astype(BF)
    ga[1, :, 256:384] = jnp.zeros((W, 128), BF)
    arrived([to(ga.at[1 - core], la_c, 0, partner)])
    for j in range(4):
        rows = pl.ds(j * 128, 128)
        ha[j] = (ga[core, rows, :].astype(F32) + la_c[rows, :].astype(F32)).astype(BF)
    wait_a = over_lat(ha, la_y, 0)

    acc_n[...] = jnp.zeros_like(acc_n)

    def back_take(k):
        @pl.when(valid(k, 1))
        def _():
            spread = place(T_DEC_NODE, k, NODES, DROWS).astype(BF)
            await_bytes(rsem, 2, k, bd)
            acc_n[...] += dot(spread, get_rows(bd, k, SD).astype(BF))

    loop(back_take)

    back_pre = acc_n[...].astype(BF)
    back_node = dot_nt(back_pre, w_msg[...])
    back_node_half = back_node.astype(BF)
    back_act = (dot_nt(back_node_half, w_down[...]) * slope(act[...])).astype(BF)
    back_norm = dot_nt(back_act, w_up[...]) * node_gain[...]
    state = nstate[...]
    inv_rms = lax.rsqrt(jnp.mean(state * state, axis=-1, keepdims=True) + 1e-05)
    mean_term = jnp.mean(state * back_norm, axis=-1, keepdims=True)
    back_state = back_node + inv_rms * back_norm - state * (inv_rms * inv_rms * inv_rms * mean_term)
    back_half = back_state.astype(BF)
    backw[...] = dot_nt(back_half, w_enc[...]).astype(BF)

    def enc_back_send(k):
        @pl.when(valid(k, -1))
        def _():
            put_rows(fs, k, dot(pick(T_ENC_NODE, k, EROWS, NODES), backw[...]), SEP)
            send(3, k, fs, fd, -1)
            own(k, fs, fd)

    loop(enc_back_send, 0, 5)

    gb[0, :, 0:512] = (dot_tn(nhalf[...], back_pre) * scale).astype(BF)
    gb[0, :, 512:1024] = (dot_tn(hidden[...], back_node_half) * scale).astype(BF)
    gb[1, :, 0:512] = (dot_tn(normed[...], back_act) * scale).astype(BF)
    gb[1, :, 512:1024] = (dot_tn(aggb[...], back_half) * scale).astype(BF)
    wait_b = [to(gb.at[1 - core], lb_c, 4, partner)]
    loop(enc_back_send, 5, 9)

    arrived(wait_b)
    for j in range(4):
        rows = pl.ds(j * 128, 128)
        both = gb[core, rows, :].astype(F32) + lb_c[rows, :].astype(F32)
        hu[j] = both[:, 0:512].astype(BF)
        for i in range(4):
            hv[i, j] = both[i * 32 : (i + 1) * 32, 512:1024].astype(BF)
    wait_u = over_lat(hu, lu_y, 4)
    wait_v = over_lon(hv, lv_z, 8)
    arrived(wait_a)
    total = ha[la].astype(F32) + la_y[0].astype(F32) + la_y[1].astype(F32) + la_y[2].astype(F32)
    for j in range(4):
        ha2[j] = total[j * 32 : (j + 1) * 32, :].astype(BF)
    wait_a = over_lon(ha2, la_z, 12)

    arrived(wait_u)
    total = hu[la].astype(F32) + lu_y[0].astype(F32) + lu_y[1].astype(F32) + lu_y[2].astype(F32)
    for j in range(4):
        hu2[j] = total[j * 32 : (j + 1) * 32, :].astype(BF)
    wait_u = over_lon(hu2, lu_z, 16)
    arrived(wait_v)
    for j in range(4):
        total = hv[lo, j].astype(F32) + lv_z[0, j].astype(F32)
        hv2[j] = (total + lv_z[1, j].astype(F32) + lv_z[2, j].astype(F32)).astype(BF)
    wait_v = over_lat(hv2, lv_y, 20)

    def finished(own_part, landed):
        total = own_part.astype(F32) + landed[0].astype(F32)
        return total + landed[1].astype(F32) + landed[2].astype(F32)

    arrived(wait_u)
    arrived(wait_v)
    arrived(wait_a)
    for at, total in (
        (0, finished(hu2[lo], lu_z)),
        (512, finished(hv2[la], lv_y)),
        (1024, finished(ha2[lo], la_z)),
    ):
        for j in range(8):
            hm[j, :, at : at + total.shape[1]] = total[j * 4 : (j + 1) * 4, :].astype(BF)
    wait_m = []
    for d in (4, 3, 5, 2, 6, 1, 7):
        part = lax.rem(me + d, 8)
        wait_m.append(to(hm.at[part], lm.at[d - 1], 32 + d, device(0, 0, part)))

    def enc_back_take(k):
        @pl.when(valid(k, 1))
        def _():
            await_bytes(rsem, 3, k, fd)
            rows = get_rows(fd, k, SEP).astype(BF)
            weight = table[pl.ds(T_ENC_SCALE + k, 1), :][:, 0:EROWS]
            spread = (place(T_ENC_CELL, k, CELLS, EROWS) * weight).astype(BF)
            grid_grad[...] += dot(spread, rows)

    loop(enc_back_take, 0, 8)

    await_bytes(rsem, 3, 4, fd)
    rows = get_rows(fd, 4, SEP).astype(BF)
    weight = table[T_ENC_SCALE + 4 : T_ENC_SCALE + 5, 0:EROWS]
    index = table[T_ENC_CELL + 4 : T_ENC_CELL + 5, 0:EROWS].astype(jnp.int32)
    leave = []
    for b in range(4):
        at = pl.ds(b * 256, 256)
        here = index == lax.broadcasted_iota(jnp.int32, (256, EROWS), 0) + b * 256
        spread = (here.astype(F32) * weight).astype(BF)
        grid_half[at, :] = (grid_grad[at, :] + dot(spread, rows)).astype(BF)
        leave.append(pltpu.make_async_copy(grid_half.at[at], grid_out.at[at], os_.at[b]))
        leave[b].start()

    arrived(wait_m)
    landed = [lm[d].astype(F32) for d in range(7)]
    same = hm[me].astype(F32)
    other = landed[0]
    same = same + landed[1] + landed[3] + landed[5]
    other = other + landed[2] + landed[4] + landed[6]
    low = jnp.where(core == 0, same, other)
    high = jnp.where(core == 0, other, same)
    g_msg[...] = low[:, 0:512]
    g_down[...] = low[:, 512:1024]
    g_dec[:, 0:384] = low[:, 1024:1408]
    g_up[...] = high[:, 0:512]
    g_enc[...] = high[:, 512:1024]
    g_dec[:, 384:512] = high[:, 1024:1152]
    g_out[...] = high[:, 1152 : 1152 + 84]

    for c in sent:
        c.wait_send()
    for c in leave:
        c.wait()

    def drain(k):
        @pl.when(valid(k, 1))
        def _():
            await_bytes(ssem, 0, k, es)
            await_bytes(ssem, 1, k, ds_)

        @pl.when(valid(k, -1))
        def _():
            await_bytes(ssem, 2, k, bs)
            await_bytes(ssem, 3, k, fs)

    loop(drain)


def scratch():
    v = pltpu.VMEM
    return [
        v((9, 8, SE), jnp.int32),
        v((9, 8, SE), jnp.int32),
        v((9, 8, SD), jnp.int32),
        v((9, 8, SD), jnp.int32),
        v((9, 8, SE), F32),
        v((9, 8, SD), F32),
        v((9, 1, 8), jnp.int32),
        v((8, 128), F32),
        v((84, CELLS), BF),
        v((84, W), BF),
        v((1, W), F32),
        v((CELLS, W), BF),
        v((NODES, W), BF),
        v((W, W), BF),
        v((W, W), BF),
        v((W, W), BF),
        v((W, W), BF),
        v((W, W), BF),
        v((128, CELLS), F32),
        v((8, 256), F32),
        v((128, 256), F32),
        v((256, 128), F32),
        v((CELLS, W), F32),
        v((CELLS, W), BF),
        v((128, W), BF),
        v((CELLS, 128), F32),
        pltpu.SemaphoreType.DMA((4,)),
        v((8, 16, 128), F32),
        v((2, 16, 128), F32),
        v((2, NODES, W), BF),
        v((18, SD, W), BF),
        v((NODES, W), BF),
        v((72, SEP, W), BF),
        v((72, SEP, W), BF),
        v((72, SD, W), BF),
        v((72, SD, W), BF),
        v((72, SD, W), BF),
        v((72, SD, W), BF),
        v((72, SEP, W), BF),
        v((72, SEP, W), BF),
        v((NODES, W), F32),
        v((CELLS, W), F32),
        v((CELLS, W), BF),
        v((CELLS, W), BF),
        v((CELLS, W), BF),
        v((CELLS, W), BF),
        v((CELLS, 128), BF),
        v((128, W), BF),
        v((NODES, W), F32),
        v((NODES, W), F32),
        v((NODES, W), BF),
        v((NODES, W), BF),
        v((NODES, W), BF),
        v((NODES, W), BF),
        v((NODES, W), BF),
        v((2, W, 384), BF),
        v((W, 384), BF),
        v((4, 128, 384), BF),
        v((3, 128, 384), BF),
        v((4, 32, 384), BF),
        v((3, 32, 384), BF),
        v((2, W, 1024), BF),
        v((W, 1024), BF),
        v((4, 128, 512), BF),
        v((3, 128, 512), BF),
        v((4, 32, 512), BF),
        v((3, 32, 512), BF),
        v((4, 4, 32, 512), BF),
        v((3, 4, 32, 512), BF),
        v((4, 32, 512), BF),
        v((3, 32, 512), BF),
        v((8, 4, 1408), BF),
        v((7, 4, 1408), BF),
        pltpu.SemaphoreType.DMA((4, 9)),
        pltpu.SemaphoreType.DMA((4, 9)),
        pltpu.SemaphoreType.DMA((40,)),
        pltpu.SemaphoreType.DMA((40,)),
        pltpu.SemaphoreType.DMA((18,)),
    ]


def on_device(
    grid_latent,
    target,
    area,
    mesh_latent,
    node_gain,
    w_enc,
    w_up,
    w_down,
    w_msg,
    w_dec,
    w_out,
    enc_cell,
    enc_live,
    enc_weight,
    enc_node,
    dec_node,
    dec_cell,
    dec_weight,
):
    vm = pl.BlockSpec(memory_space=pltpu.VMEM)
    small = jax.ShapeDtypeStruct((4, W), F32)
    any_space = pl.BlockSpec(memory_space=pl.ANY)
    rest = (small,) * 5 + (jax.ShapeDtypeStruct((4, 84), F32),)
    outs = pl.pallas_call(
        kernel,
        out_shape=(jax.ShapeDtypeStruct((CELLS, W), BF),) + rest,
        in_specs=[any_space] * 18,
        out_specs=(any_space,) + (vm,) * 6,
        scratch_shapes=scratch(),
        compiler_params=pltpu.CompilerParams(
            collective_id=0, has_side_effects=True, vmem_limit_bytes=VMEM_LIMIT
        ),
        name="step",
    )(
        enc_cell.reshape(9, 8, SE),
        enc_node.reshape(9, 8, SE),
        dec_node.reshape(9, 8, SD),
        dec_cell.reshape(9, 8, SD),
        enc_weight.reshape(9, 8, SE),
        dec_weight.reshape(9, 8, SD),
        enc_live.reshape(9, 1, 8),
        area.reshape(8, 128),
        target.T,
        w_out.T,
        node_gain.reshape(1, W),
        grid_latent,
        mesh_latent,
        w_enc,
        w_up,
        w_down,
        w_msg,
        w_dec,
    )
    return pl.pallas_call(
        finish,
        out_shape=(jax.ShapeDtypeStruct((CELLS, W), F32),) + rest,
        in_specs=[any_space] * 7,
        out_specs=(any_space,) * 7,
        scratch_shapes=[
            pltpu.VMEM((CELLS, W), BF),
            pltpu.VMEM((CELLS, W), F32),
            pltpu.VMEM((5, 4, W), F32),
            pltpu.VMEM((4, 84), F32),
            pltpu.SemaphoreType.DMA((10,)),
            pltpu.SemaphoreType.DMA((10,)),
        ],
        compiler_params=pltpu.CompilerParams(vmem_limit_bytes=VMEM_LIMIT),
        name="finish",
    )(*outs)


def finish(*refs):
    half, full, small, head, arrive, leave = refs[14:]
    blocks = [pl.ds(b * 256, 256) for b in range(4)]
    inward = [(refs[0].at[rows], half.at[rows]) for rows in blocks]
    inward += [(refs[i], small.at[i - 1]) for i in range(1, 6)] + [(refs[6], head)]
    outward = [(full.at[rows], refs[7].at[rows]) for rows in blocks]
    outward += [(small.at[i - 1], refs[7 + i]) for i in range(1, 6)] + [(head, refs[13])]
    inward = [pltpu.make_async_copy(a, b, arrive.at[i]) for i, (a, b) in enumerate(inward)]
    outward = [pltpu.make_async_copy(a, b, leave.at[i]) for i, (a, b) in enumerate(outward)]
    for copy in inward:
        copy.start()
    for i in range(10):
        inward[i].wait()
        if i < 4:
            full[blocks[i], :] = half[blocks[i], :].astype(F32)
        outward[i].start()
    for copy in outward:
        copy.wait()


def solution(mesh):
    rows = P(AXES, None)
    slots = P(AXES, None, None, None, None)
    in_specs = (
        rows,
        rows,
        P(AXES),
        rows,
        P(),
        P(),
        P(),
        P(),
        P(),
        P(),
        P(),
        slots,
        P(AXES, None, None, None),
        slots,
        slots,
        slots,
        slots,
        slots,
    )
    return jax.shard_map(
        on_device, mesh=mesh, in_specs=in_specs, out_specs=(rows,) * 7, check_vma=False
    )
```
